32 devices in a mesh: dp: 8 (over z, y), bucket: 4 (over x, core).
Axes of the slice: x: 2, y: 2, z: 4, core: 2. Of those that a mesh axis runs over, the one named last changes fastest.
Arguments:
- tokens: bfloat16 [32768, 768], P(('dp', 'bucket')), may hold values from -6 to 6
- segment: int32 [64, 512], P(('dp', 'bucket')), may hold values from 0 to 8, as said below
- pair_order: int32 [512], replicated, may hold values from 0 to 511, each once
- cotangent: bfloat16 [32768, 768], P(('dp', 'bucket')), may hold values from -6 to 6
- query_weight: bfloat16 [768, 768], replicated, may hold values from -0.21875 to 0.21875
- query_bias: float32 [768], replicated, may hold values from -3 to 3
- key_weight: bfloat16 [768, 768], replicated, may hold values from -0.21875 to 0.21875
- value_weight: bfloat16 [768, 768], replicated, may hold values from -0.21875 to 0.21875
- value_bias: float32 [768], replicated, may hold values from -3 to 3
- out_weight: bfloat16 [768, 768], replicated, may hold values from -0.875 to 0.875
- out_bias: float32 [768], replicated, may hold values from -3 to 3
- norm_gain: float32 [768], replicated, may hold values from 0.5 to 1.5
- norm_shift: float32 [768], replicated, may hold values from -2 to 2
- inner_weight: bfloat16 [768, 3072], replicated, may hold values from -0.21875 to 0.21875
- inner_bias: float32 [3072], replicated, may hold values from -3 to 3
- outer_weight: bfloat16 [3072, 768], replicated, may hold values from -0.109375 to 0.109375
- outer_bias: float32 [768], replicated, may hold values from -3 to 3
- final_gain: float32 [768], replicated, may hold values from 0.5 to 1.5
- final_shift: float32 [768], replicated, may hold values from -0.6 to 0.6
Outputs:
- layer_out: bfloat16 [32768, 768], P(('dp', 'bucket'))
- loss_value: float32 [], replicated
- tokens_grad: float32 [32768, 768], P(('dp', 'bucket'))
- dquery_weight: float32 [768, 768], replicated
- dquery_bias: float32 [768], replicated
- dkey_weight: float32 [768, 768], replicated
- dvalue_weight: float32 [768, 768], replicated
- dvalue_bias: float32 [768], replicated
- dout_weight: float32 [768, 768], replicated
- dout_bias: float32 [768], replicated
- dnorm_gain: float32 [768], replicated
- dnorm_shift: float32 [768], replicated
- dinner_weight: float32 [768, 3072], replicated
- dinner_bias: float32 [3072], replicated
- douter_weight: float32 [3072, 768], replicated
- douter_bias: float32 [768], replicated
- dfinal_gain: float32 [768], replicated
- dfinal_shift: float32 [768], replicated
The draws below stay inside these ranges and needn't reach their ends.
Inputs may be any that keep to these rules, and one draw needn't show every extreme that they name: In each packed row the segment numbers never fall; sentences 0 to 7 each hold one or more consecutive positions, then padding holds 8. Rows on devices whose bucket index is in the upper half hold sentences of up to 64 positions, the others of up to 32, and sentence 0 of every row has exactly that most. `pair_order`: A permutation of the sentences.
All inputs are finite; a program needn't handle non-finite values.
Results may differ from the reference program's by a relative error of at most 0.012.
Values sent between devices are 32-bit elements; how exact they have to be, the bound alone decides.
A program may use at most 256 MiB of HBM per device.

```python
from functools import partial
import jax
import jax.numpy as jnp
from jax import lax

D = 768
H = 12
HD = 64
FF = 3072
L = 512
S_ROW = 8
ROWS_DEV = 2
ROWS = 64
TOKENS = 32768
SENTS = 512
PAIRS = 256
N_BUCKET = 4


def draw_segment(key, part):
    longest = L // S_ROW
    row_ids = jnp.arange(ROWS, dtype=jnp.int32)
    bucket_of = row_ids // ROWS_DEV % N_BUCKET
    most = jnp.where(bucket_of >= N_BUCKET // 2, longest, longest // 2).astype(jnp.int32)
    least = jnp.maximum(most // 2, 1)
    spread = jax.random.randint(key, (ROWS, S_ROW), 0, 1 << 20).astype(jnp.int32)
    lengths = least[:, None] + spread % (most - least + 1)[:, None]
    lengths = lengths.at[:, 0].set(most)
    ends = jnp.cumsum(lengths, axis=1).astype(jnp.int32)
    places = jnp.arange(L, dtype=jnp.int32)
    return jnp.sum((places[None, :, None] >= ends[:, None, :]).astype(jnp.int32), axis=2).astype(jnp.int32)


def block_scale(stream_key, extent, split, smallest, high):
    factor_of = 1.0
    for dim, parts in split:
        draws = jax.random.uniform(jax.random.fold_in(jax.random.fold_in(stream_key, 6), dim), (parts,), jnp.float32, smallest / len(split), high / len(split))
        factor_of = factor_of * jnp.repeat(jnp.exp(draws), extent[dim] // parts).reshape((-1,) + (1,) * (len(extent) - 1 - dim))
    return factor_of


def scatter_about(rng, shape, scale, bound, pieces=(), kind=jnp.bfloat16):
    level = block_scale(rng, shape, pieces, -0.22, 0.18) if pieces else 1.0
    drawn = jax.random.normal(rng, shape, jnp.float32) * scale * level
    return jnp.minimum(jnp.maximum(drawn, -bound), bound).astype(kind)


def setup_inputs(seed: int = 0) -> dict:
    key_of = jax.random.split(jax.random.key(seed), 20)
    tokens = scatter_about(key_of[0], (TOKENS, D), 1.0, 6.0, ((0, 32),))
    segment = draw_segment(jax.random.fold_in(key_of[19], 71), 0)
    pair_order = jax.random.permutation(key_of[2], SENTS).astype(jnp.int32)
    cotangent = scatter_about(key_of[3], (TOKENS, D), 1.0, 6.0, ((0, 32),))
    query_weight = scatter_about(key_of[4], (D, D), D ** -0.5, 0.21875)
    query_bias = scatter_about(key_of[5], (D,), 0.5, 3.0, (), jnp.float32)
    key_weight = scatter_about(key_of[6], (D, D), D ** -0.5, 0.21875)
    value_weight = scatter_about(key_of[7], (D, D), D ** -0.5, 0.21875)
    value_bias = scatter_about(key_of[8], (D,), 0.5, 3.0, (), jnp.float32)
    out_weight = scatter_about(key_of[9], (D, D), (D // 16) ** -0.5, 0.875)
    out_bias = scatter_about(key_of[10], (D,), 0.5, 3.0, (), jnp.float32)
    norm_gain = jnp.clip(1.0 + 0.1 * jax.random.normal(key_of[11], (D,), jnp.float32), 0.5, 1.5)
    norm_shift = scatter_about(key_of[12], (D,), 0.3, 2.0, (), jnp.float32)
    inner_weight = scatter_about(key_of[13], (D, FF), D ** -0.5, 0.21875)
    inner_bias = scatter_about(key_of[14], (FF,), 0.5, 3.0, (), jnp.float32)
    outer_weight = scatter_about(key_of[15], (FF, D), FF ** -0.5, 0.109375)
    outer_bias = scatter_about(key_of[16], (D,), 0.5, 3.0, (), jnp.float32)
    final_gain = jnp.clip(1.0 + 0.1 * jax.random.normal(key_of[17], (D,), jnp.float32), 0.5, 1.5)
    final_shift = scatter_about(key_of[18], (D,), 0.1, 0.6, (), jnp.float32)
    return {"tokens": tokens, "segment": segment, "pair_order": pair_order, "cotangent": cotangent, "query_weight": query_weight, "query_bias": query_bias, "key_weight": key_weight, "value_weight": value_weight, "value_bias": value_bias, "out_weight": out_weight, "out_bias": out_bias, "norm_gain": norm_gain, "norm_shift": norm_shift, "inner_weight": inner_weight, "inner_bias": inner_bias, "outer_weight": outer_weight, "outer_bias": outer_bias, "final_gain": final_gain, "final_shift": final_shift}


@jax.custom_vjp
def low(v):
    return lax.optimization_barrier(v.astype(jnp.bfloat16)).astype(jnp.float32)

@jax.custom_vjp
def low_back(v):
    return v

def low_keep(v):
    return (low(v), None)

def low_pass(kept, grad):
    return (grad,)

def back_keep(v):
    return (v, None)

def back_low(kept, grad):
    return (low(grad),)
low.defvjp(low_keep, low_pass)
low_back.defvjp(back_keep, back_low)

def matmul(left, right):
    return jnp.dot(left, right, precision=lax.Precision.HIGHEST, preferred_element_type=jnp.float32)

def layer_norm(hidden, gain, shift):
    centred = hidden - lax.optimization_barrier(jnp.mean(hidden, axis=-1, keepdims=True))
    spread = lax.rsqrt(lax.optimization_barrier(jnp.mean(centred * centred, axis=-1, keepdims=True)) + 1e-05)
    return centred * spread * gain + shift

def rows_forward(params, group):
    query_weight, query_bias, key_weight, value_weight, value_bias, out_weight, out_bias, norm_gain, norm_shift, inner_weight, inner_bias, outer_weight, outer_bias, final_gain, final_shift = params
    block_x, block_seg = group
    nrows = block_x.shape[0]
    inputs = block_x.reshape(nrows * L, D)
    inputs_b = low(inputs)
    query = low(low_back(matmul(inputs_b, query_weight)) + query_bias).reshape(nrows, L, H, HD)
    keys = low(low_back(matmul(inputs_b, key_weight))).reshape(nrows, L, H, HD)
    values = low(low_back(matmul(inputs_b, value_weight)) + value_bias).reshape(nrows, L, H, HD)
    raw = jnp.einsum('rqhe,rkhe->rhqk', query, keys, precision=lax.Precision.HIGHEST)
    scores = low_back(0.125 * raw)
    same = block_seg[:, None, :, None] == block_seg[:, None, None, :]
    scores = jnp.where(same, scores, jnp.float32(-1000000000.0))
    probs = low(jax.nn.softmax(scores, axis=-1))
    context = jnp.einsum('rhqk,rkhe->rqhe', probs, values, precision=lax.Precision.HIGHEST)
    context = low(low_back(context)).reshape(nrows * L, D)
    first = inputs + low_back(matmul(context, out_weight)) + out_bias
    normed = layer_norm(first, norm_gain, norm_shift)
    normed_b = low(normed)
    inner = low_back(matmul(normed_b, inner_weight)) + inner_bias
    active = low(jax.nn.gelu(inner, approximate=False))
    second = normed + low_back(matmul(active, outer_weight)) + outer_bias
    final = layer_norm(second, final_gain, final_shift)
    return final.reshape(nrows, L, D)

def reference(tokens, segment, pair_order, cotangent, query_weight, query_bias, key_weight, value_weight, value_bias, out_weight, out_bias, norm_gain, norm_shift, inner_weight, inner_bias, outer_weight, outer_bias, final_gain, final_shift):
    inputs = tokens.astype(jnp.float32)
    weights = tuple((w.astype(jnp.float32) for w in (query_weight, query_bias, key_weight, value_weight, value_bias, out_weight, out_bias, norm_gain, norm_shift, inner_weight, inner_bias, outer_weight, outer_bias, final_gain, final_shift)))
    upstream = cotangent.astype(jnp.float32).reshape(ROWS, L, D)
    groups = ROWS // 8

    def objective(inputs, *params):
        block = jax.checkpoint(partial(rows_forward, params))
        final = lax.map(block, (inputs.reshape(groups, 8, L, D), segment.reshape(groups, 8, L)))
        final = final.reshape(ROWS, L, D)
        onehot = (segment[:, None, :] == jnp.arange(S_ROW, dtype=jnp.int32)[None, :, None]).astype(jnp.float32)
        counts = lax.optimization_barrier(jnp.sum(onehot, axis=2))
        pooled = jnp.einsum('rsl,rld->rsd', onehot, final, precision=lax.Precision.HIGHEST) / counts[:, :, None]
        pooled = pooled.reshape(SENTS, D)
        ordered = pooled[pair_order]
        anchors = ordered[:PAIRS]
        positives = ordered[PAIRS:]
        unit_a = anchors * lax.rsqrt(lax.optimization_barrier(jnp.sum(anchors * anchors, axis=1, keepdims=True)) + 1e-06)
        unit_p = positives * lax.rsqrt(lax.optimization_barrier(jnp.sum(positives * positives, axis=1, keepdims=True)) + 1e-06)
        logits = 20.0 * matmul(unit_a, unit_p.T)
        loss = jnp.sum(jax.nn.logsumexp(logits, axis=1) - jnp.diagonal(logits))
        total = loss + jnp.sum(upstream * final)
        return (total, (final, loss))
    total, back, aux = jax.vjp(objective, inputs, *weights, has_aux=True)
    final, loss = aux
    grads = back(jnp.ones_like(total))
    return (final.reshape(TOKENS, D).astype(jnp.bfloat16), loss, grads[0], grads[1], grads[2], grads[3], grads[4], grads[5], grads[6], grads[7], grads[8], grads[9], grads[10], grads[11], grads[12], grads[13], grads[14], grads[15])
```

```python
import functools

import jax
import jax.numpy as jnp
from jax import lax
from jax.experimental import pallas as pl
from jax.experimental.pallas import tpu as pltpu
from jax.sharding import PartitionSpec as P

H = 12
HD = 64
S_ROW = 8

MESH = pl.DeviceIdType.MESH

norm_eps = 1e-05
cos_scale = 20.0
masked_score = -1000000000.0


def layer_norm(hidden, gain, shift):
    centred = hidden - jnp.mean(hidden, axis=-1, keepdims=True)
    spread = lax.rsqrt(jnp.mean(centred * centred, axis=-1, keepdims=True) + norm_eps)
    return centred * spread * gain + shift


def gelu_exact(values):
    return jax.nn.gelu(values, approximate=False)


def matmul(left, right):
    return jnp.dot(left, right, preferred_element_type=jnp.float32)


def matmul_left(left, right):
    return lax.dot_general(
        left, right, (((0,), (0,)), ((), ())), preferred_element_type=jnp.float32
    )


def matmul_right(left, right):
    return lax.dot_general(
        left, right, (((1,), (1,)), ((), ())), preferred_element_type=jnp.float32
    )


def exact_dot(left, right, dims):
    return lax.dot_general(
        left,
        right,
        (dims, ((), ())),
        precision=lax.Precision.HIGHEST,
        preferred_element_type=jnp.float32,
    )


def to_sphere(vectors):
    factor = lax.rsqrt(jnp.sum(vectors * vectors, axis=1, keepdims=True) + 1e-06)
    return (vectors * factor, factor)


def sphere_back(unit, factor, upstream):
    return factor * (upstream - unit * jnp.sum(unit * upstream, axis=1, keepdims=True))


def masked_scores(query_h, key_h, same):
    raw = jnp.einsum("rqhe,rkhe->rhqk", query_h, key_h, preferred_element_type=jnp.float32) * 0.125
    return jnp.where(same, raw, jnp.float32(masked_score))


def row_logsum(logits):
    top = jnp.max(logits, axis=1, keepdims=True)
    return top + jnp.log(jnp.sum(jnp.exp(logits - top), axis=1, keepdims=True))


def bit_dims(dp_size, bucket_size):
    dims = []
    for axis, size in ((1, bucket_size), (0, dp_size)):
        bit = 1
        while bit < size:
            dims.append((axis, bit))
            bit *= 2
    return dims

class Route:
    def __init__(self, dims):
        self.dims = dims
        self.pos = (lax.axis_index("dp"), lax.axis_index("bucket"))
        self.bits = [(self.pos[a] // b) % 2 for a, b in dims]

    def weights(self, stage, colour=0):
        core = self.bits[0]
        n = len(self.dims)
        if stage == 0 or n < 3:
            return {stage: 1}
        if n != 5 or isinstance(colour, int):
            if stage in (1, 2):
                return {stage: 1 - core, 3 - stage: core}
            return {stage: 1}
        keep = 1 - colour
        table = {
            1: {1: keep * (1 - core), 2: keep * core, 3: colour},
            2: {2: keep * (1 - core), 1: keep * core, 4: colour},
            3: {3: keep, 1: colour * (1 - core), 2: colour * core},
            4: {4: keep, 2: colour * (1 - core), 1: colour * core},
        }
        return table[stage]

    def bit(self, stage, colour=0):
        w = self.weights(stage, colour)
        return sum(v * self.bits[k] for k, v in w.items())

    def partner(self, stage, colour=0):
        where = list(self.pos)
        for k, v in self.weights(stage, colour).items():
            axis, bit = self.dims[k]
            where[axis] = where[axis] + v * (bit * (1 - 2 * self.bits[k]))
        return tuple(where)

def colour_of(c):
    return 1 - ((2 * c) % 9 + 7) // 9

def ar_kernel(dims, nblk, colours, *refs):
    ins = refs[:6]
    vec_in, out, vec_out, grads = refs[6:10]
    S = len(dims)
    stages = refs[10:10 + S]
    vbuf, vrecv, isem, ssem, rsem, osem, vs, vr, freed = refs[10 + S:]
    blk = grads.shape[1]
    rows = grads.shape[0]
    CH = 8 << S
    C = rows // CH
    width = grads.shape[1]
    route = Route(dims)
    bar = pltpu.get_barrier_semaphore()
    for k in range(S):
        axis, bit = dims[k]
        where = list(route.pos)
        where[axis] = where[axis] + bit * (1 - 2 * route.bits[k])
        pl.semaphore_signal(bar, inc=1, device_id=tuple(where), device_id_type=MESH)
    srcs = []
    for r in ins:
        h, w = r.shape
        for i in range(h // blk):
            for j in range(w // width):
                srcs.append(r.at[pl.ds(i * blk, blk), pl.ds(j * width, width)])
    for b, s in enumerate(srcs):
        pltpu.make_async_copy(s, grads.at[pl.ds(b * blk, blk)], isem.at[b]).start()
    vbuf[0] = vec_in[...]
    pl.semaphore_wait(bar, S)

    def col(c):
        return colour_of(c) if colours else 0
    def base(s, c):
        o = c * CH
        for k in range(s):
            o = o + route.bit(k, col(c)) * (CH >> (k + 1))
        return o
    def rs(s, c):
        half = CH >> (s + 1)
        b = route.bit(s, col(c))
        o = base(s, c)
        keep = pl.multiple_of(o + b * half, 8)
        send = pl.multiple_of(o + (1 - b) * half, 8)
        land = pl.multiple_of(c * half, 8)
        cp = pltpu.make_async_remote_copy(grads.at[pl.ds(send, half)], stages[s].at[pl.ds(land, half)],
            ssem.at[s, c], rsem.at[s, c], device_id=route.partner(s, col(c)), device_id_type=MESH)
        return cp, keep, land, half
    def ag(s, c):
        half = CH >> (s + 1)
        keep = pl.multiple_of(base(s, c) + route.bit(s, col(c)) * half, 8)
        return pltpu.make_async_remote_copy(grads.at[pl.ds(keep, half)], grads.at[pl.ds(keep, half)],
            ssem.at[2 * S - 1 - s, c], rsem.at[2 * S - 1 - s, c], device_id=route.partner(s, col(c)), device_id_type=MESH)
    def outc(c):
        o = pl.multiple_of(c * CH, 8)
        return pltpu.make_async_copy(grads.at[pl.ds(o, CH)], out.at[pl.ds(o, CH)], osem.at[c])
    def need(c):
        return ((c + 1) * CH + blk - 1) // blk
    def start(p, c):
        if p == 0:
            def w(b, _):
                pltpu.make_async_copy(srcs[0], grads.at[pl.ds(pl.multiple_of(b * blk, 8), blk)], isem.at[b]).wait()
                return 0
            lo = need(c - 1)
            lax.fori_loop(lo, need(c), w, 0)
        if p < S:
            rs(p, c)[0].start()
        elif p < 2 * S:
            pl.semaphore_wait(freed.at[2 * S - 1 - p, c], 1)
            ag(2 * S - 1 - p, c).start()
        else:
            outc(c).start()
    def finish(p, c):
        if p < S:
            cp, keep, land, half = rs(p, c)
            cp.wait_recv()
            grads[pl.ds(keep, half)] = grads[pl.ds(keep, half)] + stages[p][pl.ds(land, half)]
            cp.wait_send()
            pl.semaphore_signal(freed.at[p, c], inc=1, device_id=route.partner(p, col(c)), device_id_type=MESH)
        elif p < 2 * S:
            ag(2 * S - 1 - p, c).wait()
        else:
            outc(c).wait()
    def vcopy(r):
        axis, bit = dims[r]
        where = list(route.pos)
        where[axis] = where[axis] + bit * (1 - 2 * route.bits[r])
        return pltpu.make_async_remote_copy(vbuf.at[r], vrecv.at[r], vs.at[r], vr.at[r], device_id=tuple(where), device_id_type=MESH)
    NP = 2 * S + 1
    def step(t, _):
        for p in range(NP):
            c = t - 2 * p
            @pl.when((c >= 0) & (c < C))
            def _():
                start(p, c)
        for r in range(S):
            @pl.when(t == 2 + 2 * r)
            def _():
                vcopy(r).start()
        for p in range(NP):
            c = t - 1 - 2 * p
            @pl.when((c >= 0) & (c < C))
            def _():
                finish(p, c)
        for r in range(S):
            @pl.when(t == 3 + 2 * r)
            def _():
                cp = vcopy(r)
                cp.wait()
                vbuf[r + 1] = vbuf[r] + vrecv[r]
        return 0
    lax.fori_loop(0, C + 2 * (NP - 1) + 1, step, 0)
    vec_out[...] = vbuf[S]

def all_reduce(parts, vec, dp_size, bucket_size, colours=False):
    dims = bit_dims(dp_size, bucket_size)
    S = len(dims)
    width = parts[0].shape[1]
    rows = sum(p.size for p in parts) // width
    nblk = rows // width
    CH = 8 << S
    f32 = jnp.float32
    any_spec = pl.BlockSpec(memory_space=pl.ANY)
    vm = pl.BlockSpec(memory_space=pltpu.VMEM)
    return pl.pallas_call(
        functools.partial(ar_kernel, dims, nblk, colours),
        out_shape=(jax.ShapeDtypeStruct((rows, width), f32), jax.ShapeDtypeStruct(vec.shape, f32)),
        in_specs=[any_spec] * 6 + [vm], out_specs=(any_spec, vm),
        scratch_shapes=[pltpu.VMEM((rows, width), f32)]
        + [pltpu.VMEM((rows >> (s + 1), width), f32) for s in range(S)]
        + [pltpu.VMEM((S + 1,) + vec.shape, f32), pltpu.VMEM((S,) + vec.shape, f32),
           pltpu.SemaphoreType.DMA((nblk,)), pltpu.SemaphoreType.DMA((2 * S, rows // CH)), pltpu.SemaphoreType.DMA((2 * S, rows // CH)),
           pltpu.SemaphoreType.DMA((rows // CH,)), pltpu.SemaphoreType.DMA((S,)), pltpu.SemaphoreType.DMA((S,)),
           pltpu.SemaphoreType.REGULAR((S, rows // CH))],
        compiler_params=pltpu.CompilerParams(collective_id=1, has_side_effects=True, vmem_limit_bytes=67043328),
    )(*parts, vec)


def local(
    dp_size,
    bucket_size,
    tokens,
    segment,
    pair_order,
    cotangent,
    query_weight,
    query_bias,
    key_weight,
    value_weight,
    value_bias,
    out_weight,
    out_bias,
    norm_gain,
    norm_shift,
    inner_weight,
    inner_bias,
    outer_weight,
    outer_bias,
    final_gain,
    final_shift,
):
    nrows = segment.shape[0]
    seqlen = segment.shape[1]
    width = tokens.shape[1]
    query_b = (matmul(tokens, query_weight) + query_bias).astype(jnp.bfloat16)
    key_b = matmul(tokens, key_weight).astype(jnp.bfloat16)
    value_b = (matmul(tokens, value_weight) + value_bias).astype(jnp.bfloat16)
    query_h = query_b.reshape(nrows, seqlen, H, HD)
    key_h = key_b.reshape(nrows, seqlen, H, HD)
    value_h = value_b.reshape(nrows, seqlen, H, HD)
    same = segment[:, None, :, None] == segment[:, None, None, :]
    scores = masked_scores(query_h, key_h, same)
    peak = jnp.max(scores, axis=-1, keepdims=True)
    log_total = peak + jnp.log(jnp.sum(jnp.exp(scores - peak), axis=-1, keepdims=True))
    probs_b = jnp.exp(scores - log_total).astype(jnp.bfloat16)
    context = jnp.einsum("rhqk,rkhe->rqhe", probs_b, value_h, preferred_element_type=jnp.float32)
    context_b = context.astype(jnp.bfloat16).reshape(nrows * seqlen, width)
    first = tokens.astype(jnp.float32) + matmul(context_b, out_weight) + out_bias
    normed, norm_back = jax.vjp(layer_norm, first, norm_gain, norm_shift)
    normed_b = normed.astype(jnp.bfloat16)
    inner = matmul(normed_b, inner_weight) + inner_bias
    active, gelu_back = jax.vjp(gelu_exact, inner)
    active_b = active.astype(jnp.bfloat16)
    second = normed + matmul(active_b, outer_weight) + outer_bias
    final, final_back = jax.vjp(layer_norm, second, final_gain, final_shift)
    layer_out = final.astype(jnp.bfloat16)
    onehot = (segment[:, None, :] == jnp.arange(S_ROW, dtype=jnp.int32)[None, :, None]).astype(
        jnp.float32
    )
    counts = jnp.sum(onehot, axis=2, keepdims=True)
    pooled = (
        jnp.einsum(
            "rsl,rld->rsd",
            onehot,
            final.reshape(nrows, seqlen, width),
            precision=lax.Precision.HIGHEST,
        )
        / counts
    )
    pooled = pooled.reshape(nrows * S_ROW, width)
    pooled_every = lax.all_gather(pooled, ("dp", "bucket"), axis=0, tiled=True)
    sents = pooled_every.shape[0]
    pairs = sents // 2
    device = lax.axis_index(("dp", "bucket"))
    unit, factor = to_sphere(pooled_every[pair_order])
    unit_a, unit_p = unit[:pairs], unit[pairs:]
    logits = cos_scale * exact_dot(unit_a, unit_p, ((1,), (1,)))
    log_sum = row_logsum(logits)
    columns = jnp.arange(pairs, dtype=jnp.int32)[None, :]
    on_diagonal = (columns == columns.T).astype(jnp.float32)
    loss_value = jnp.sum(log_sum[:, 0] - jnp.sum(logits * on_diagonal, axis=1))
    weighting = jnp.exp(logits - log_sum) - on_diagonal
    mine = device * nrows * S_ROW + jnp.arange(nrows * S_ROW, dtype=jnp.int32)
    pick = (mine[:, None] == pair_order[None, :]).astype(jnp.float32)
    row_part = exact_dot(pick[:, :pairs], weighting, ((1,), (0,)))
    column_part = exact_dot(pick[:, pairs:], weighting, ((1,), (1,)))
    grad_unit = cos_scale * (
        exact_dot(row_part, unit_p, ((1,), (0,))) + exact_dot(column_part, unit_a, ((1,), (0,)))
    )
    unit_own, factor_own = to_sphere(pooled)
    dpooled = sphere_back(unit_own, factor_own, grad_unit)
    spread_back = jnp.einsum(
        "rsl,rsd->rld",
        onehot,
        dpooled.reshape(nrows, S_ROW, width) / counts,
        precision=lax.Precision.HIGHEST,
    )
    grad_final = cotangent.astype(jnp.float32) + spread_back.reshape(nrows * seqlen, width)
    grad_second, dfinal_gain, dfinal_shift = final_back(grad_final)
    grad_second_b = grad_second.astype(jnp.bfloat16)
    douter_weight = matmul_left(active_b, grad_second_b)
    douter_bias = jnp.sum(grad_second, axis=0)
    (grad_inner,) = gelu_back(matmul_right(grad_second_b, outer_weight))
    grad_inner_b = grad_inner.astype(jnp.bfloat16)
    dinner_weight = matmul_left(normed_b, grad_inner_b)
    dinner_bias = jnp.sum(grad_inner, axis=0)
    grad_normed = grad_second + matmul_right(grad_inner_b, inner_weight)
    grad_first, dnorm_gain, dnorm_shift = norm_back(grad_normed)
    grad_first_b = grad_first.astype(jnp.bfloat16)
    dout_weight = matmul_left(context_b, grad_first_b)
    dout_bias = jnp.sum(grad_first, axis=0)
    grad_context = (
        matmul_right(grad_first_b, out_weight).astype(jnp.bfloat16).reshape(nrows, seqlen, H, HD)
    )
    scores = masked_scores(query_h, key_h, same)
    probs = jnp.exp(scores - log_total)
    probs_b = probs.astype(jnp.bfloat16)
    grad_probs = jnp.einsum(
        "rqhe,rkhe->rhqk", grad_context, value_h, preferred_element_type=jnp.float32
    )
    grad_value = jnp.einsum(
        "rhqk,rqhe->rkhe", probs_b, grad_context, preferred_element_type=jnp.float32
    )
    grad_scores = probs * (grad_probs - jnp.sum(probs * grad_probs, axis=-1, keepdims=True))
    grad_scores_b = grad_scores.astype(jnp.bfloat16)
    grad_query = (
        jnp.einsum("rhqk,rkhe->rqhe", grad_scores_b, key_h, preferred_element_type=jnp.float32)
        * 0.125
    )
    grad_key = (
        jnp.einsum("rhqk,rqhe->rkhe", grad_scores_b, query_h, preferred_element_type=jnp.float32)
        * 0.125
    )
    grad_query = grad_query.reshape(nrows * seqlen, width)
    grad_key = grad_key.reshape(nrows * seqlen, width)
    grad_value = grad_value.reshape(nrows * seqlen, width)
    dquery_bias = jnp.sum(grad_query, axis=0)
    dvalue_bias = jnp.sum(grad_value, axis=0)
    grad_query_b = grad_query.astype(jnp.bfloat16)
    grad_key_b = grad_key.astype(jnp.bfloat16)
    grad_value_b = grad_value.astype(jnp.bfloat16)
    dquery_weight = matmul_left(tokens, grad_query_b)
    dkey_weight = matmul_left(tokens, grad_key_b)
    dvalue_weight = matmul_left(tokens, grad_value_b)
    tokens_grad = (
        grad_first
        + matmul_right(grad_query_b, query_weight)
        + matmul_right(grad_key_b, key_weight)
        + matmul_right(grad_value_b, value_weight)
    )
    vectors = [
        dquery_bias, dvalue_bias, dout_bias, dnorm_gain, dnorm_shift,
        dinner_bias, douter_bias, dfinal_gain, dfinal_shift,
    ]
    packed = jnp.concatenate(vectors).reshape(-1, width)
    nvec = packed.shape[0]
    packed = jnp.pad(packed, ((0, -nvec % 8), (0, 0)))
    flat, packed = all_reduce(
        [douter_weight, dinner_weight, dout_weight, dquery_weight, dkey_weight, dvalue_weight],
        packed, dp_size, bucket_size,
    )
    blocks = flat.reshape(-1, width, width)
    wide = inner_weight.shape[1] // width
    douter_weight = flat[: wide * width]
    dinner_weight = jnp.concatenate([blocks[wide + j] for j in range(wide)], axis=1)
    dout_weight, dquery_weight, dkey_weight, dvalue_weight = (blocks[2 * wide + j] for j in range(4))
    packed = packed[:nvec].reshape(-1)
    sizes = [v.shape[0] for v in vectors]
    ends = [sum(sizes[: i + 1]) for i in range(len(sizes))]
    (
        dquery_bias, dvalue_bias, dout_bias, dnorm_gain, dnorm_shift,
        dinner_bias, douter_bias, dfinal_gain, dfinal_shift,
    ) = (packed[e - n : e] for e, n in zip(ends, sizes))
    return (
        layer_out,
        loss_value,
        tokens_grad,
        dquery_weight,
        dquery_bias,
        dkey_weight,
        dvalue_weight,
        dvalue_bias,
        dout_weight,
        dout_bias,
        dnorm_gain,
        dnorm_shift,
        dinner_weight,
        dinner_bias,
        douter_weight,
        douter_bias,
        dfinal_gain,
        dfinal_shift,
    )


def solution(mesh):
    return jax.shard_map(
        functools.partial(local, mesh.shape["dp"], mesh.shape["bucket"]),
        mesh=mesh,
        in_specs=(
            P(("dp", "bucket"), None),
            P(("dp", "bucket"), None),
            P(),
            P(("dp", "bucket"), None),
            P(),
            P(),
            P(),
            P(),
            P(),
            P(),
            P(),
            P(),
            P(),
            P(),
            P(),
            P(),
            P(),
            P(),
            P(),
        ),
        out_specs=(
            P(("dp", "bucket"), None),
            P(),
            P(("dp", "bucket"), None),
            P(),
            P(),
            P(),
            P(),
            P(),
            P(),
            P(),
            P(),
            P(),
            P(),
            P(),
            P(),
            P(),
            P(),
            P(),
        ),
        check_vma=False,
    )
```

```python
import functools

import jax
import jax.numpy as jnp
import numpy as np
from jax import lax
from jax.experimental import pallas as pl
from jax.experimental.pallas import tpu as pltpu
from jax.sharding import PartitionSpec as P

H = 12
HD = 64
S_ROW = 8
norm_eps = 1e-05
masked_score = -1000000000.0
BF = jnp.bfloat16
F32 = jnp.float32
HIGH = lax.Precision.HIGHEST


def dot(a, b, da, db, precision=None):
    return lax.dot_general(
        a, b, (((da,), (db,)), ((), ())), precision=precision, preferred_element_type=F32
    )


def halves(width=128):
    lane = lax.broadcasted_iota(jnp.int32, (1, width), 1)
    low = (lane < width // 2).astype(F32)
    return low.astype(BF), (1.0 - low).astype(BF)


def normalise(hidden):
    centred = hidden - jnp.mean(hidden, axis=-1, keepdims=True)
    rate = lax.rsqrt(jnp.mean(centred * centred, axis=-1, keepdims=True) + norm_eps)
    return centred * rate, rate


def forward_kernel(
    x_in, seg_row, seg_col, wq_h, bq, wk_h, wv_h, bv, wo_h, bo, g1, s1, wi_h, bi, w2_h, b2, g2, s2,
    q_o, k_o, v_o, c_o, nb_o, z1_o, r1_o, act_o, dg_o, z2_o, r2_o, lse_o, out_o, pool_o,
    wq, wk, wv, wo, wi, w2, q, k, v, ctx, nf, nb, z1, r1, act, dg, z2, r2, fin, lout, bias,
    wsem, osem,
):
    rows, width = x_in.shape
    nrow = seg_row.shape[0]
    seqlen = rows // nrow
    pairs = width // 128
    inner = wi.shape[1]
    TM = 256
    loads = [
        pltpu.make_async_copy(a, b, wsem.at[i])
        for i, (a, b) in enumerate(
            [(wq_h, wq), (wk_h, wk), (wv_h, wv), (wo_h, wo), (wi_h, wi), (w2_h, w2)]
        )
    ]
    for c in loads:
        c.start()
    stores = []

    def put(i, src, dst):
        c = pltpu.make_async_copy(src, dst, osem.at[i])
        c.start()
        stores.append(c)

    def tile(i):
        return pl.ds(pl.multiple_of(i * TM, TM), TM)

    for c in loads[:3]:
        c.wait()

    def project(i, _):
        x = x_in[tile(i)]
        q[tile(i)] = (dot(x, wq[...], 1, 0) + bq[...]).astype(BF)
        k[tile(i)] = dot(x, wk[...], 1, 0).astype(BF)
        v[tile(i)] = (dot(x, wv[...], 1, 0) + bv[...]).astype(BF)
        return 0

    lax.fori_loop(0, rows // TM, project, 0)
    put(0, q, q_o)
    put(1, k, k_o)
    put(2, v, v_o)
    parts = halves()

    def row(r, _):
        span = pl.ds(pl.multiple_of(r * seqlen, seqlen), seqlen)
        same = seg_col[span] == seg_row[r]
        bias[...] = jnp.where(same, 0.0, masked_score).astype(F32)

        def pair(p, _):
            lanes = pl.ds(pl.multiple_of(p * 128, 128), 128)
            qp = q[span, lanes] * jnp.asarray(0.125, BF)
            kp = k[span, lanes]
            vp = v[span, lanes]
            total = None
            for half, part in enumerate(parts):
                s = dot(kp * part, qp, 1, 1) + bias[...]
                top = jnp.max(s, axis=0, keepdims=True)
                e = jnp.exp(s - top)
                mass = jnp.sum(e, axis=0, keepdims=True)
                prob = (e * (1.0 / mass)).astype(BF)
                c = dot(vp * part, prob, 0, 0)
                total = c if total is None else total + c
                lse_o[r * pairs * 2 + p * 2 + half] = top + jnp.log(mass)
            ctx[span, lanes] = total.T.astype(BF)
            return 0

        lax.fori_loop(0, pairs, pair, 0)
        return 0

    lax.fori_loop(0, nrow, row, 0)
    put(3, ctx, c_o)
    loads[3].wait()

    def attend(i, _):
        first = x_in[tile(i)].astype(F32) + dot(ctx[tile(i)], wo[...], 1, 0) + bo[...]
        z, rate = normalise(first)
        normed = z * g1[...] + s1[...]
        nf[tile(i)] = normed
        nb[tile(i)] = normed.astype(BF)
        z1[tile(i)] = z.astype(BF)
        r1[tile(i)] = jnp.broadcast_to(rate, (TM, 128))
        return 0

    lax.fori_loop(0, rows // TM, attend, 0)
    put(4, nb, nb_o)
    put(5, z1, z1_o)
    put(6, r1, r1_o)
    loads[4].wait()
    loads[5].wait()
    TF = 512

    def feed(i, _):
        def block(j, _):
            cols = pl.ds(pl.multiple_of(j * TF, TF), TF)
            h = dot(nb[tile(i)], wi[:, cols], 1, 0) + bi[:, cols]
            cdf = 0.5 + 0.5 * lax.erf(h * 0.7071067811865476)
            act_b = (h * cdf).astype(BF)
            act[tile(i), cols] = act_b
            slope = cdf + h * (0.3989422804014327 * jnp.exp(-0.5 * h * h))
            dg[tile(i), cols] = slope.astype(BF)
            return 0

        lax.fori_loop(0, inner // TF, block, 0)
        second = nf[tile(i)] + dot(act[tile(i)], w2[...], 1, 0) + b2[...]
        z, rate = normalise(second)
        final = z * g2[...] + s2[...]
        fin[tile(i)] = final
        lout[tile(i)] = final.astype(BF)
        z2[tile(i)] = z.astype(BF)
        r2[tile(i)] = jnp.broadcast_to(rate, (TM, 128))
        return 0

    lax.fori_loop(0, rows // TM, feed, 0)
    put(7, act, act_o)
    put(8, dg, dg_o)
    put(9, z2, z2_o)
    put(10, r2, r2_o)
    put(11, lout, out_o)
    for r in range(nrow):
        kinds = lax.broadcasted_iota(jnp.int32, (S_ROW, seqlen), 0)
        onehot = (seg_row[r] == kinds).astype(F32)
        count = jnp.sum(onehot, axis=1, keepdims=True)
        got = dot(onehot, fin[r * seqlen : (r + 1) * seqlen], 1, 0, HIGH)
        pool_o[r * S_ROW : (r + 1) * S_ROW] = got / count
    for c in stores:
        c.wait()


def forward(tokens, segment, wq, bq, wk, wv, bv, wo, bo, g1, s1, wi, bi, w2, b2, g2, s2):
    rows, width = tokens.shape
    nrow, seqlen = segment.shape
    inner = wi.shape[1]
    heads = width // 64
    vm = pl.BlockSpec(memory_space=pltpu.VMEM)
    hbm = pl.BlockSpec(memory_space=pl.ANY)
    act = (rows, width)
    wide = (rows, inner)
    sd = jax.ShapeDtypeStruct
    outs = (
        sd(act, BF), sd(act, BF), sd(act, BF), sd(act, BF), sd(act, BF), sd(act, BF),
        sd((rows, 128), F32), sd(wide, BF), sd(wide, BF), sd(act, BF), sd((rows, 128), F32),
        sd((nrow * heads, 1, seqlen), F32), sd(act, BF), sd((nrow * S_ROW, width), F32),
    )
    row = lambda a: a.reshape(1, -1)
    return pl.pallas_call(
        forward_kernel,
        name="forward",
        out_shape=outs,
        in_specs=[vm, vm, vm, hbm, vm, hbm, hbm, vm, hbm, vm, vm, vm, hbm, vm, hbm, vm, vm, vm],
        out_specs=[hbm] * 11 + [vm, hbm, vm],
        scratch_shapes=[pltpu.VMEM((width, width), BF)] * 4
        + [pltpu.VMEM((width, inner), BF), pltpu.VMEM((inner, width), BF)]
        + [pltpu.VMEM(act, BF)] * 4
        + [pltpu.VMEM(act, F32), pltpu.VMEM(act, BF), pltpu.VMEM(act, BF), pltpu.VMEM((rows, 128), F32)]
        + [pltpu.VMEM(wide, BF), pltpu.VMEM(wide, BF), pltpu.VMEM(act, BF), pltpu.VMEM((rows, 128), F32)]
        + [pltpu.VMEM(act, F32), pltpu.VMEM(act, BF), pltpu.VMEM((seqlen, seqlen), F32)]
        + [pltpu.SemaphoreType.DMA((6,)), pltpu.SemaphoreType.DMA((12,))],
        compiler_params=pltpu.CompilerParams(vmem_limit_bytes=64000000),
    )(
        tokens, segment.reshape(nrow, 1, seqlen), segment.reshape(rows, 1), wq, row(bq), wk, wv,
        row(bv), wo, row(bo), row(g1), row(s1), wi, row(bi), w2, row(b2), row(g2), row(s2),
    )


MESH = pl.DeviceIdType.MESH

def bit_dims(dp_size, bucket_size):
    dims = []
    for axis, size in ((1, bucket_size), (0, dp_size)):
        bit = 1
        while bit < size:
            dims.append((axis, bit))
            bit *= 2
    return dims

class Route:
    def __init__(self, dims):
        self.dims = dims
        self.pos = (lax.axis_index("dp"), lax.axis_index("bucket"))
        self.bits = [(self.pos[a] // b) % 2 for a, b in dims]

    def weights(self, stage, colour=0):
        core = self.bits[0]
        n = len(self.dims)
        if stage == 0 or n < 3:
            return {stage: 1}
        if n != 5 or isinstance(colour, int):
            if stage in (1, 2):
                return {stage: 1 - core, 3 - stage: core}
            return {stage: 1}
        keep = 1 - colour
        table = {
            1: {1: keep * (1 - core), 2: keep * core, 3: colour},
            2: {2: keep * (1 - core), 1: keep * core, 4: colour},
            3: {3: keep, 1: colour * (1 - core), 2: colour * core},
            4: {4: keep, 2: colour * (1 - core), 1: colour * core},
        }
        return table[stage]

    def bit(self, stage, colour=0):
        w = self.weights(stage, colour)
        return sum(v * self.bits[k] for k, v in w.items())

    def partner(self, stage, colour=0):
        where = list(self.pos)
        for k, v in self.weights(stage, colour).items():
            axis, bit = self.dims[k]
            where[axis] = where[axis] + v * (bit * (1 - 2 * self.bits[k]))
        return tuple(where)

def colour_of(c):
    return 1 - ((2 * c) % 9 + 7) // 9

def ar_kernel(dims, nblk, colours, *refs):
    ins = refs[:6]
    vec_in, out, vec_out, grads = refs[6:10]
    S = len(dims)
    stages = refs[10:10 + S]
    vbuf, vrecv, isem, ssem, rsem, osem, vs, vr, freed = refs[10 + S:]
    blk = grads.shape[1]
    rows = grads.shape[0]
    CH = 8 << S
    C = rows // CH
    width = grads.shape[1]
    route = Route(dims)
    bar = pltpu.get_barrier_semaphore()
    for k in range(S):
        axis, bit = dims[k]
        where = list(route.pos)
        where[axis] = where[axis] + bit * (1 - 2 * route.bits[k])
        pl.semaphore_signal(bar, inc=1, device_id=tuple(where), device_id_type=MESH)
    srcs = []
    for r in ins:
        h, w = r.shape
        for i in range(h // blk):
            for j in range(w // width):
                srcs.append(r.at[pl.ds(i * blk, blk), pl.ds(j * width, width)])
    for b, s in enumerate(srcs):
        pltpu.make_async_copy(s, grads.at[pl.ds(b * blk, blk)], isem.at[b]).start()
    vbuf[0] = vec_in[...]
    pl.semaphore_wait(bar, S)

    def col(c):
        return colour_of(c) if colours else 0
    def base(s, c):
        o = c * CH
        for k in range(s):
            o = o + route.bit(k, col(c)) * (CH >> (k + 1))
        return o
    def rs(s, c):
        half = CH >> (s + 1)
        b = route.bit(s, col(c))
        o = base(s, c)
        keep = pl.multiple_of(o + b * half, 8)
        send = pl.multiple_of(o + (1 - b) * half, 8)
        land = pl.multiple_of(c * half, 8)
        cp = pltpu.make_async_remote_copy(grads.at[pl.ds(send, half)], stages[s].at[pl.ds(land, half)],
            ssem.at[s, c], rsem.at[s, c], device_id=route.partner(s, col(c)), device_id_type=MESH)
        return cp, keep, land, half
    def ag(s, c):
        half = CH >> (s + 1)
        keep = pl.multiple_of(base(s, c) + route.bit(s, col(c)) * half, 8)
        return pltpu.make_async_remote_copy(grads.at[pl.ds(keep, half)], grads.at[pl.ds(keep, half)],
            ssem.at[2 * S - 1 - s, c], rsem.at[2 * S - 1 - s, c], device_id=route.partner(s, col(c)), device_id_type=MESH)
    def outc(c):
        o = pl.multiple_of(c * CH, 8)
        return pltpu.make_async_copy(grads.at[pl.ds(o, CH)], out.at[pl.ds(o, CH)], osem.at[c])
    def need(c):
        return ((c + 1) * CH + blk - 1) // blk
    def start(p, c):
        if p == 0:
            def w(b, _):
                pltpu.make_async_copy(srcs[0], grads.at[pl.ds(pl.multiple_of(b * blk, 8), blk)], isem.at[b]).wait()
                return 0
            lo = need(c - 1)
            lax.fori_loop(lo, need(c), w, 0)
        if p < S:
            rs(p, c)[0].start()
        elif p < 2 * S:
            pl.semaphore_wait(freed.at[2 * S - 1 - p, c], 1)
            ag(2 * S - 1 - p, c).start()
        else:
            outc(c).start()
    def finish(p, c):
        if p < S:
            cp, keep, land, half = rs(p, c)
            cp.wait_recv()
            grads[pl.ds(keep, half)] = grads[pl.ds(keep, half)] + stages[p][pl.ds(land, half)]
            cp.wait_send()
            pl.semaphore_signal(freed.at[p, c], inc=1, device_id=route.partner(p, col(c)), device_id_type=MESH)
        elif p < 2 * S:
            ag(2 * S - 1 - p, c).wait()
        else:
            outc(c).wait()
    def vcopy(r):
        axis, bit = dims[r]
        where = list(route.pos)
        where[axis] = where[axis] + bit * (1 - 2 * route.bits[r])
        return pltpu.make_async_remote_copy(vbuf.at[r], vrecv.at[r], vs.at[r], vr.at[r], device_id=tuple(where), device_id_type=MESH)
    NP = 2 * S + 1
    def step(t, _):
        for p in range(NP):
            c = t - 2 * p
            @pl.when((c >= 0) & (c < C))
            def _():
                start(p, c)
        for r in range(S):
            @pl.when(t == 2 + 2 * r)
            def _():
                vcopy(r).start()
        for p in range(NP):
            c = t - 1 - 2 * p
            @pl.when((c >= 0) & (c < C))
            def _():
                finish(p, c)
        for r in range(S):
            @pl.when(t == 3 + 2 * r)
            def _():
                cp = vcopy(r)
                cp.wait()
                vbuf[r + 1] = vbuf[r] + vrecv[r]
        return 0
    lax.fori_loop(0, C + 2 * (NP - 1) + 1, step, 0)
    vec_out[...] = vbuf[S]

def all_reduce(parts, vec, dp_size, bucket_size, colours=False):
    dims = bit_dims(dp_size, bucket_size)
    S = len(dims)
    width = parts[0].shape[1]
    rows = sum(p.size for p in parts) // width
    nblk = rows // width
    CH = 8 << S
    f32 = jnp.float32
    any_spec = pl.BlockSpec(memory_space=pl.ANY)
    vm = pl.BlockSpec(memory_space=pltpu.VMEM)
    return pl.pallas_call(
        functools.partial(ar_kernel, dims, nblk, colours),
        out_shape=(jax.ShapeDtypeStruct((rows, width), f32), jax.ShapeDtypeStruct(vec.shape, f32)),
        in_specs=[any_spec] * 6 + [vm], out_specs=(any_spec, vm),
        scratch_shapes=[pltpu.VMEM((rows, width), f32)]
        + [pltpu.VMEM((rows >> (s + 1), width), f32) for s in range(S)]
        + [pltpu.VMEM((S + 1,) + vec.shape, f32), pltpu.VMEM((S,) + vec.shape, f32),
           pltpu.SemaphoreType.DMA((nblk,)), pltpu.SemaphoreType.DMA((2 * S, rows // CH)), pltpu.SemaphoreType.DMA((2 * S, rows // CH)),
           pltpu.SemaphoreType.DMA((rows // CH,)), pltpu.SemaphoreType.DMA((S,)), pltpu.SemaphoreType.DMA((S,)),
           pltpu.SemaphoreType.REGULAR((S, rows // CH))],
        compiler_params=pltpu.CompilerParams(collective_id=1, has_side_effects=True, vmem_limit_bytes=67043328),
    )(*parts, vec)


cos_scale = 20.0


def gather_order(dims, dp_size, bucket_size, own):
    S = len(dims)
    n = np.arange(dp_size * bucket_size)
    key = [(n >> (S - 1 - s)) & 1 for s in range(S)]
    if S >= 3:
        core = key[0]
        key[1], key[2] = np.where(core == 1, key[2], key[1]), np.where(core == 1, key[1], key[2])
    pos = [0, 0]
    for (axis, bit), value in zip(dims, key):
        pos[axis] = pos[axis] + bit * value
    device = pos[0] * bucket_size + pos[1]
    return (device[:, None] * own + np.arange(own)[None, :]).reshape(1, -1).astype(np.int32)


def sphere(vectors):
    factor = lax.rsqrt(jnp.sum(vectors * vectors, axis=1, keepdims=True) + 1e-06)
    return vectors * factor, factor


def loss_kernel(dims, bucket_size, pool, sid, pair_row, pair_col, dpool, loss, buf, unit, weigh, ssem, rsem):
    own, width = pool.shape
    sents = buf.shape[0]
    pairs = sents // 2
    S = len(dims)
    route = Route(dims)
    bar = pltpu.get_barrier_semaphore()
    for k in range(S):
        axis, bit = dims[k]
        where = list(route.pos)
        where[axis] = where[axis] + bit * (1 - 2 * route.bits[k])
        pl.semaphore_signal(bar, inc=1, device_id=tuple(where), device_id_type=MESH)
    base = [0]
    for s in range(S):
        base.append(base[s] + route.bit(s) * (sents >> (s + 1)))
    buf[pl.ds(pl.multiple_of(base[S], 8), own)] = pool[...]
    pl.semaphore_wait(bar, S)
    for s in reversed(range(S)):
        half = sents >> (s + 1)
        here = pl.ds(pl.multiple_of(base[s + 1], 8), half)
        c = pltpu.make_async_remote_copy(
            buf.at[here], buf.at[here], ssem.at[s], rsem.at[s],
            device_id=route.partner(s), device_id_type=MESH,
        )
        c.start()
        c.wait()
    B = min(256, pairs)
    for i in range(sents // B):
        part = pl.ds(i * B, B)
        pick = (pair_col[part] == sid[...]).astype(F32)
        ordered = dot(pick, buf[...], 1, 0, HIGH)
        unit[part] = sphere(ordered)[0]
    total = jnp.zeros((1, 1), F32)
    for i in range(pairs // B):
        part = pl.ds(i * B, B)
        logits = cos_scale * dot(unit[part], unit[pairs:], 1, 1, HIGH)
        top = jnp.max(logits, axis=1, keepdims=True)
        row_lse = top + jnp.log(jnp.sum(jnp.exp(logits - top), axis=1, keepdims=True))
        line = lax.broadcasted_iota(jnp.int32, logits.shape, 0) + i * B
        eye = (line == lax.broadcasted_iota(jnp.int32, logits.shape, 1)).astype(F32)
        weigh[part] = jnp.exp(logits - row_lse) - eye
        gap = row_lse - jnp.sum(logits * eye, axis=1, keepdims=True)
        total = total + jnp.sum(gap, axis=0, keepdims=True)
    loss[...] = total
    first = (route.pos[0] * bucket_size + route.pos[1]) * own
    mine = lax.broadcasted_iota(jnp.int32, (own, sents), 0) + first
    choose = (mine == pair_row[...]).astype(F32)
    by_row = dot(choose[:, :pairs], weigh[...], 1, 0, HIGH)
    by_column = dot(choose[:, pairs:], weigh[...], 1, 1, HIGH)
    grad = cos_scale * (dot(by_row, unit[pairs:], 1, 0, HIGH) + dot(by_column, unit[:pairs], 1, 0, HIGH))
    u, factor = sphere(pool[...])
    dpool[...] = factor * (grad - u * jnp.sum(u * grad, axis=1, keepdims=True))


def pair_loss(pool, pair_order, dp_size, bucket_size):
    dims = bit_dims(dp_size, bucket_size)
    S = len(dims)
    own, width = pool.shape
    sents = pair_order.shape[0]
    vm = pl.BlockSpec(memory_space=pltpu.VMEM)
    sid = jnp.asarray(gather_order(dims, dp_size, bucket_size, own))
    return pl.pallas_call(
        functools.partial(loss_kernel, dims, bucket_size),
        name="pair_loss",
        out_shape=(jax.ShapeDtypeStruct(pool.shape, F32), jax.ShapeDtypeStruct((1, 1), F32)),
        in_specs=[vm] * 4, out_specs=(vm, vm),
        scratch_shapes=[
            pltpu.VMEM((sents, width), F32), pltpu.VMEM((sents, width), F32),
            pltpu.VMEM((sents // 2, sents // 2), F32),
            pltpu.SemaphoreType.DMA((S,)), pltpu.SemaphoreType.DMA((S,)),
        ],
        compiler_params=pltpu.CompilerParams(collective_id=2, has_side_effects=True, vmem_limit_bytes=60000000),
    )(pool, sid, pair_order.reshape(1, -1), pair_order.reshape(-1, 1))


def norm_grad(dx, z, rate, gain):
    dz = dx * gain
    mean = jnp.mean(dz, axis=-1, keepdims=True)
    cross = jnp.mean(dz * z, axis=-1, keepdims=True)
    return rate * (dz - mean - z * cross), jnp.sum(dx * z, axis=0), jnp.sum(dx, axis=0)


def local(
    dp_size, bucket_size,
    tokens, segment, pair_order, cotangent, query_weight, query_bias, key_weight, value_weight,
    value_bias, out_weight, out_bias, norm_gain, norm_shift, inner_weight, inner_bias,
    outer_weight, outer_bias, final_gain, final_shift,
):
    nrows, seqlen = segment.shape
    width = tokens.shape[1]
    (
        query_b, key_b, value_b, context_b, normed_b, z1, r1, active_b, slope, z2, r2, lse,
        layer_out, pooled,
    ) = forward(
        tokens, segment, query_weight, query_bias, key_weight, value_weight, value_bias,
        out_weight, out_bias, norm_gain, norm_shift, inner_weight, inner_bias, outer_weight,
        outer_bias, final_gain, final_shift,
    )
    dpooled, loss_value = pair_loss(pooled, pair_order, dp_size, bucket_size)
    loss_value = loss_value.reshape(())
    onehot = (segment[:, None, :] == jnp.arange(S_ROW, dtype=jnp.int32)[None, :, None]).astype(F32)
    counts = jnp.sum(onehot, axis=2, keepdims=True)
    spread = jnp.einsum(
        "rsl,rsd->rld", onehot, dpooled.reshape(nrows, S_ROW, width) / counts, precision=HIGH
    )
    grad_final = cotangent.astype(F32) + spread.reshape(nrows * seqlen, width)
    grad_second, dfinal_gain, dfinal_shift = norm_grad(
        grad_final, z2.astype(F32), r2[:, :1], final_gain
    )
    grad_second_b = grad_second.astype(BF)
    douter_weight = dot(active_b, grad_second_b, 0, 0)
    douter_bias = jnp.sum(grad_second, axis=0)
    grad_inner = dot(grad_second_b, outer_weight, 1, 1) * slope.astype(F32)
    grad_inner_b = grad_inner.astype(BF)
    dinner_weight = dot(normed_b, grad_inner_b, 0, 0)
    dinner_bias = jnp.sum(grad_inner, axis=0)
    grad_normed = grad_second + dot(grad_inner_b, inner_weight, 1, 1)
    grad_first, dnorm_gain, dnorm_shift = norm_grad(
        grad_normed, z1.astype(F32), r1[:, :1], norm_gain
    )
    grad_first_b = grad_first.astype(BF)
    dout_weight = dot(context_b, grad_first_b, 0, 0)
    dout_bias = jnp.sum(grad_first, axis=0)
    split = lambda a: a.reshape(nrows, seqlen, H, HD)
    grad_context = split(dot(grad_first_b, out_weight, 1, 1).astype(BF))
    query_h, key_h, value_h = split(query_b), split(key_b), split(value_b)
    same = segment[:, None, :, None] == segment[:, None, None, :]
    ein = functools.partial(jnp.einsum, preferred_element_type=F32)
    scores = jnp.where(same, ein("rqhe,rkhe->rhqk", query_h, key_h) * 0.125, masked_score)
    probs = jnp.exp(scores - lse.reshape(nrows, H, seqlen, 1))
    probs_b = probs.astype(BF)
    grad_probs = ein("rqhe,rkhe->rhqk", grad_context, value_h)
    grad_value = ein("rhqk,rqhe->rkhe", probs_b, grad_context)
    grad_scores = probs * (grad_probs - jnp.sum(probs * grad_probs, axis=-1, keepdims=True))
    grad_scores_b = grad_scores.astype(BF)
    grad_query = ein("rhqk,rkhe->rqhe", grad_scores_b, key_h) * 0.125
    grad_key = ein("rhqk,rqhe->rkhe", grad_scores_b, query_h) * 0.125
    grad_query = grad_query.reshape(nrows * seqlen, width)
    grad_key = grad_key.reshape(nrows * seqlen, width)
    grad_value = grad_value.reshape(nrows * seqlen, width)
    dquery_bias = jnp.sum(grad_query, axis=0)
    dvalue_bias = jnp.sum(grad_value, axis=0)
    grad_query_b = grad_query.astype(BF)
    grad_key_b = grad_key.astype(BF)
    grad_value_b = grad_value.astype(BF)
    dquery_weight = dot(tokens, grad_query_b, 0, 0)
    dkey_weight = dot(tokens, grad_key_b, 0, 0)
    dvalue_weight = dot(tokens, grad_value_b, 0, 0)
    tokens_grad = (
        grad_first
        + dot(grad_query_b, query_weight, 1, 1)
        + dot(grad_key_b, key_weight, 1, 1)
        + dot(grad_value_b, value_weight, 1, 1)
    )
    vectors = [
        dquery_bias, dvalue_bias, dout_bias, dnorm_gain, dnorm_shift,
        dinner_bias, douter_bias, dfinal_gain, dfinal_shift,
    ]
    packed = jnp.concatenate(vectors).reshape(-1, width)
    nvec = packed.shape[0]
    packed = jnp.pad(packed, ((0, -nvec % 8), (0, 0)))
    flat, packed = all_reduce(
        [douter_weight, dinner_weight, dout_weight, dquery_weight, dkey_weight, dvalue_weight],
        packed, dp_size, bucket_size, True,
    )
    blocks = flat.reshape(-1, width, width)
    wide = inner_weight.shape[1] // width
    douter_weight = flat[: wide * width]
    dinner_weight = jnp.concatenate([blocks[wide + j] for j in range(wide)], axis=1)
    dout_weight, dquery_weight, dkey_weight, dvalue_weight = (blocks[2 * wide + j] for j in range(4))
    packed = packed[:nvec].reshape(-1)
    sizes = [v.shape[0] for v in vectors]
    ends = [sum(sizes[: i + 1]) for i in range(len(sizes))]
    (
        dquery_bias, dvalue_bias, dout_bias, dnorm_gain, dnorm_shift,
        dinner_bias, douter_bias, dfinal_gain, dfinal_shift,
    ) = (packed[e - n : e] for e, n in zip(ends, sizes))
    return (
        layer_out, loss_value, tokens_grad, dquery_weight, dquery_bias, dkey_weight,
        dvalue_weight, dvalue_bias, dout_weight, dout_bias, dnorm_gain, dnorm_shift,
        dinner_weight, dinner_bias, douter_weight, douter_bias, dfinal_gain, dfinal_shift,
    )


def solution(mesh):
    split = P(("dp", "bucket"), None)
    return jax.shard_map(
        functools.partial(local, mesh.shape["dp"], mesh.shape["bucket"]),
        mesh=mesh,
        in_specs=(split, split, P(), split) + (P(),) * 15,
        out_specs=(split, P(), split) + (P(),) * 15,
        check_vma=False,
    )
```

```python
import functools

import jax
import jax.numpy as jnp
import numpy as np
from jax import lax
from jax.experimental import pallas as pl
from jax.experimental.pallas import tpu as pltpu
from jax.sharding import PartitionSpec as P

H = 12
HD = 64
S_ROW = 8
norm_eps = 1e-05
masked_score = -1000000000.0
BF = jnp.bfloat16
F32 = jnp.float32
HIGH = lax.Precision.HIGHEST


def dot(a, b, da, db, precision=None):
    return lax.dot_general(
        a, b, (((da,), (db,)), ((), ())), precision=precision, preferred_element_type=F32
    )


def halves(width=128):
    lane = lax.broadcasted_iota(jnp.int32, (1, width), 1)
    low = (lane < width // 2).astype(F32)
    return low.astype(BF), (1.0 - low).astype(BF)


def normalise(hidden):
    centred = hidden - jnp.mean(hidden, axis=-1, keepdims=True)
    rate = lax.rsqrt(jnp.mean(centred * centred, axis=-1, keepdims=True) + norm_eps)
    return centred * rate, rate


def forward_kernel(
    x_in, seg_row, seg_col, wq_h, bq, wk_h, wv_h, bv, wo_h, bo, g1, s1, wi_h, bi, w2_h, b2, g2, s2,
    q_o, k_o, v_o, c_o, nb_o, z1_o, r1_o, act_o, dg_o, z2_o, r2_o, lse_o, out_o, pool_o,
    wq, wk, wv, wo, wi, w2, q, k, v, ctx, nf, nb, z1, r1, act, dg, z2, r2, fin, lout, bias,
    wsem, osem,
):
    rows, width = x_in.shape
    nrow = seg_row.shape[0]
    seqlen = rows // nrow
    pairs = width // 128
    inner = wi.shape[1]
    TM = 256
    loads = [
        pltpu.make_async_copy(a, b, wsem.at[i])
        for i, (a, b) in enumerate(
            [(wq_h, wq), (wk_h, wk), (wv_h, wv), (wo_h, wo), (wi_h, wi), (w2_h, w2)]
        )
    ]
    for c in loads:
        c.start()
    stores = []

    def put(i, src, dst):
        c = pltpu.make_async_copy(src, dst, osem.at[i])
        c.start()
        stores.append(c)

    def tile(i):
        return pl.ds(pl.multiple_of(i * TM, TM), TM)

    for c in loads[:3]:
        c.wait()

    def project(i, _):
        x = x_in[tile(i)]
        q[tile(i)] = (dot(x, wq[...], 1, 0) + bq[...]).astype(BF)
        k[tile(i)] = dot(x, wk[...], 1, 0).astype(BF)
        v[tile(i)] = (dot(x, wv[...], 1, 0) + bv[...]).astype(BF)
        return 0

    lax.fori_loop(0, rows // TM, project, 0)
    put(0, q, q_o)
    put(1, k, k_o)
    put(2, v, v_o)
    parts = halves()

    def row(r, _):
        span = pl.ds(pl.multiple_of(r * seqlen, seqlen), seqlen)
        same = seg_col[span] == seg_row[r]
        bias[...] = jnp.where(same, 0.0, masked_score).astype(F32)

        def pair(p, _):
            lanes = pl.ds(pl.multiple_of(p * 128, 128), 128)
            qp = q[span, lanes] * jnp.asarray(0.125, BF)
            kp = k[span, lanes]
            vp = v[span, lanes]
            total = None
            for half, part in enumerate(parts):
                s = dot(kp * part, qp, 1, 1) + bias[...]
                top = jnp.max(s, axis=0, keepdims=True)
                e = jnp.exp(s - top)
                mass = jnp.sum(e, axis=0, keepdims=True)
                prob = (e * (1.0 / mass)).astype(BF)
                c = dot(vp * part, prob, 0, 0)
                total = c if total is None else total + c
                lse_o[r * pairs * 2 + p * 2 + half] = top + jnp.log(mass)
            ctx[span, lanes] = total.T.astype(BF)
            return 0

        lax.fori_loop(0, pairs, pair, 0)
        return 0

    lax.fori_loop(0, nrow, row, 0)
    put(3, ctx, c_o)
    loads[3].wait()

    def attend(i, _):
        first = x_in[tile(i)].astype(F32) + dot(ctx[tile(i)], wo[...], 1, 0) + bo[...]
        z, rate = normalise(first)
        normed = z * g1[...] + s1[...]
        nf[tile(i)] = normed
        nb[tile(i)] = normed.astype(BF)
        z1[tile(i)] = z.astype(BF)
        r1[tile(i)] = jnp.broadcast_to(rate, (TM, 128))
        return 0

    lax.fori_loop(0, rows // TM, attend, 0)
    put(4, nb, nb_o)
    put(5, z1, z1_o)
    put(6, r1, r1_o)
    loads[4].wait()
    loads[5].wait()
    TF = 512

    def feed(i, _):
        def block(j, _):
            cols = pl.ds(pl.multiple_of(j * TF, TF), TF)
            h = dot(nb[tile(i)], wi[:, cols], 1, 0) + bi[:, cols]
            cdf = 0.5 + 0.5 * lax.erf(h * 0.7071067811865476)
            act_b = (h * cdf).astype(BF)
            act[tile(i), cols] = act_b
            slope = cdf + h * (0.3989422804014327 * jnp.exp(-0.5 * h * h))
            dg[tile(i), cols] = slope.astype(BF)
            return 0

        lax.fori_loop(0, inner // TF, block, 0)
        second = nf[tile(i)] + dot(act[tile(i)], w2[...], 1, 0) + b2[...]
        z, rate = normalise(second)
        final = z * g2[...] + s2[...]
        fin[tile(i)] = final
        lout[tile(i)] = final.astype(BF)
        z2[tile(i)] = z.astype(BF)
        r2[tile(i)] = jnp.broadcast_to(rate, (TM, 128))
        return 0

    lax.fori_loop(0, rows // TM, feed, 0)
    put(7, act, act_o)
    put(8, dg, dg_o)
    put(9, z2, z2_o)
    put(10, r2, r2_o)
    put(11, lout, out_o)
    for r in range(nrow):
        kinds = lax.broadcasted_iota(jnp.int32, (S_ROW, seqlen), 0)
        onehot = (seg_row[r] == kinds).astype(F32)
        count = jnp.sum(onehot, axis=1, keepdims=True)
        got = dot(onehot, fin[r * seqlen : (r + 1) * seqlen], 1, 0, HIGH)
        pool_o[r * S_ROW : (r + 1) * S_ROW] = got / count
    for c in stores:
        c.wait()


def forward(tokens, segment, wq, bq, wk, wv, bv, wo, bo, g1, s1, wi, bi, w2, b2, g2, s2):
    rows, width = tokens.shape
    nrow, seqlen = segment.shape
    inner = wi.shape[1]
    heads = width // 64
    vm = pl.BlockSpec(memory_space=pltpu.VMEM)
    hbm = pl.BlockSpec(memory_space=pl.ANY)
    act = (rows, width)
    wide = (rows, inner)
    sd = jax.ShapeDtypeStruct
    outs = (
        sd(act, BF), sd(act, BF), sd(act, BF), sd(act, BF), sd(act, BF), sd(act, BF),
        sd((rows, 128), F32), sd(wide, BF), sd(wide, BF), sd(act, BF), sd((rows, 128), F32),
        sd((nrow * heads, 1, seqlen), F32), sd(act, BF), sd((nrow * S_ROW, width), F32),
    )
    row = lambda a: a.reshape(1, -1)
    return pl.pallas_call(
        forward_kernel,
        name="forward",
        out_shape=outs,
        in_specs=[vm, vm, vm, hbm, vm, hbm, hbm, vm, hbm, vm, vm, vm, hbm, vm, hbm, vm, vm, vm],
        out_specs=[hbm] * 11 + [vm, hbm, vm],
        scratch_shapes=[pltpu.VMEM((width, width), BF)] * 4
        + [pltpu.VMEM((width, inner), BF), pltpu.VMEM((inner, width), BF)]
        + [pltpu.VMEM(act, BF)] * 4
        + [pltpu.VMEM(act, F32), pltpu.VMEM(act, BF), pltpu.VMEM(act, BF), pltpu.VMEM((rows, 128), F32)]
        + [pltpu.VMEM(wide, BF), pltpu.VMEM(wide, BF), pltpu.VMEM(act, BF), pltpu.VMEM((rows, 128), F32)]
        + [pltpu.VMEM(act, F32), pltpu.VMEM(act, BF), pltpu.VMEM((seqlen, seqlen), F32)]
        + [pltpu.SemaphoreType.DMA((6,)), pltpu.SemaphoreType.DMA((12,))],
        compiler_params=pltpu.CompilerParams(vmem_limit_bytes=64000000),
    )(
        tokens, segment.reshape(nrow, 1, seqlen), segment.reshape(rows, 1), wq, row(bq), wk, wv,
        row(bv), wo, row(bo), row(g1), row(s1), wi, row(bi), w2, row(b2), row(g2), row(s2),
    )


MESH = pl.DeviceIdType.MESH

def bit_dims(dp_size, bucket_size):
    dims = []
    for axis, size in ((1, bucket_size), (0, dp_size)):
        bit = 1
        while bit < size:
            dims.append((axis, bit))
            bit *= 2
    return dims

class Route:
    def __init__(self, dims):
        self.dims = dims
        self.pos = (lax.axis_index("dp"), lax.axis_index("bucket"))
        self.bits = [(self.pos[a] // b) % 2 for a, b in dims]

    def weights(self, stage, colour=0):
        core = self.bits[0]
        n = len(self.dims)
        if stage == 0 or n < 3:
            return {stage: 1}
        if n != 5 or isinstance(colour, int):
            if stage in (1, 2):
                return {stage: 1 - core, 3 - stage: core}
            return {stage: 1}
        keep = 1 - colour
        table = {
            1: {1: keep * (1 - core), 2: keep * core, 3: colour},
            2: {2: keep * (1 - core), 1: keep * core, 4: colour},
            3: {3: keep, 1: colour * (1 - core), 2: colour * core},
            4: {4: keep, 2: colour * (1 - core), 1: colour * core},
        }
        return table[stage]

    def bit(self, stage, colour=0):
        w = self.weights(stage, colour)
        return sum(v * self.bits[k] for k, v in w.items())

    def partner(self, stage, colour=0):
        where = list(self.pos)
        for k, v in self.weights(stage, colour).items():
            axis, bit = self.dims[k]
            where[axis] = where[axis] + v * (bit * (1 - 2 * self.bits[k]))
        return tuple(where)

def colour_of(c):
    return 1 - ((2 * c) % 9 + 7) // 9


cos_scale = 20.0


def gather_order(dims, dp_size, bucket_size, own):
    S = len(dims)
    n = np.arange(dp_size * bucket_size)
    key = [(n >> (S - 1 - s)) & 1 for s in range(S)]
    if S >= 3:
        core = key[0]
        key[1], key[2] = np.where(core == 1, key[2], key[1]), np.where(core == 1, key[1], key[2])
    pos = [0, 0]
    for (axis, bit), value in zip(dims, key):
        pos[axis] = pos[axis] + bit * value
    device = pos[0] * bucket_size + pos[1]
    return (device[:, None] * own + np.arange(own)[None, :]).reshape(1, -1).astype(np.int32)


def sphere(vectors):
    factor = lax.rsqrt(jnp.sum(vectors * vectors, axis=1, keepdims=True) + 1e-06)
    return vectors * factor, factor


def loss_kernel(dims, bucket_size, pool, sid, pair_row, pair_col, dpool, loss, buf, unit, weigh, ssem, rsem):
    own, width = pool.shape
    sents = buf.shape[0]
    pairs = sents // 2
    S = len(dims)
    route = Route(dims)
    bar = pltpu.get_barrier_semaphore()
    for k in range(S):
        axis, bit = dims[k]
        where = list(route.pos)
        where[axis] = where[axis] + bit * (1 - 2 * route.bits[k])
        pl.semaphore_signal(bar, inc=1, device_id=tuple(where), device_id_type=MESH)
    base = [0]
    for s in range(S):
        base.append(base[s] + route.bit(s) * (sents >> (s + 1)))
    buf[pl.ds(pl.multiple_of(base[S], 8), own)] = pool[...]
    pl.semaphore_wait(bar, S)
    for s in reversed(range(S)):
        half = sents >> (s + 1)
        here = pl.ds(pl.multiple_of(base[s + 1], 8), half)
        c = pltpu.make_async_remote_copy(
            buf.at[here], buf.at[here], ssem.at[s], rsem.at[s],
            device_id=route.partner(s), device_id_type=MESH,
        )
        c.start()
        c.wait()
    B = min(256, pairs)
    for i in range(sents // B):
        part = pl.ds(i * B, B)
        pick = (pair_col[part] == sid[...]).astype(F32)
        ordered = dot(pick, buf[...], 1, 0, HIGH)
        unit[part] = sphere(ordered)[0]
    total = jnp.zeros((1, 1), F32)
    for i in range(pairs // B):
        part = pl.ds(i * B, B)
        logits = cos_scale * dot(unit[part], unit[pairs:], 1, 1, HIGH)
        top = jnp.max(logits, axis=1, keepdims=True)
        row_lse = top + jnp.log(jnp.sum(jnp.exp(logits - top), axis=1, keepdims=True))
        line = lax.broadcasted_iota(jnp.int32, logits.shape, 0) + i * B
        eye = (line == lax.broadcasted_iota(jnp.int32, logits.shape, 1)).astype(F32)
        weigh[part] = jnp.exp(logits - row_lse) - eye
        gap = row_lse - jnp.sum(logits * eye, axis=1, keepdims=True)
        total = total + jnp.sum(gap, axis=0, keepdims=True)
    loss[...] = total
    first = (route.pos[0] * bucket_size + route.pos[1]) * own
    mine = lax.broadcasted_iota(jnp.int32, (own, sents), 0) + first
    choose = (mine == pair_row[...]).astype(F32)
    by_row = dot(choose[:, :pairs], weigh[...], 1, 0, HIGH)
    by_column = dot(choose[:, pairs:], weigh[...], 1, 1, HIGH)
    grad = cos_scale * (dot(by_row, unit[pairs:], 1, 0, HIGH) + dot(by_column, unit[:pairs], 1, 0, HIGH))
    u, factor = sphere(pool[...])
    dpool[...] = factor * (grad - u * jnp.sum(u * grad, axis=1, keepdims=True))


def pair_loss(pool, pair_order, dp_size, bucket_size):
    dims = bit_dims(dp_size, bucket_size)
    S = len(dims)
    own, width = pool.shape
    sents = pair_order.shape[0]
    vm = pl.BlockSpec(memory_space=pltpu.VMEM)
    sid = jnp.asarray(gather_order(dims, dp_size, bucket_size, own))
    return pl.pallas_call(
        functools.partial(loss_kernel, dims, bucket_size),
        name="pair_loss",
        out_shape=(jax.ShapeDtypeStruct(pool.shape, F32), jax.ShapeDtypeStruct((1, 1), F32)),
        in_specs=[vm] * 4, out_specs=(vm, vm),
        scratch_shapes=[
            pltpu.VMEM((sents, width), F32), pltpu.VMEM((sents, width), F32),
            pltpu.VMEM((sents // 2, sents // 2), F32),
            pltpu.SemaphoreType.DMA((S,)), pltpu.SemaphoreType.DMA((S,)),
        ],
        compiler_params=pltpu.CompilerParams(collective_id=2, has_side_effects=True, vmem_limit_bytes=60000000),
    )(pool, sid, pair_order.reshape(1, -1), pair_order.reshape(-1, 1))


UNIT = 256


def norm_grad(dx, z, rate, gain):
    dz = dx * gain
    mean = jnp.mean(dz, axis=-1, keepdims=True)
    cross = jnp.mean(dz * z, axis=-1, keepdims=True)
    dh = rate * (dz - mean - z * cross)
    return dh, jnp.sum(dx * z, axis=0, keepdims=True), jnp.sum(dx, axis=0, keepdims=True)


def backward_kernel(
    dims,
    x_h, cot_h, q_h, k_h, v_h, c_h, nb_h, z1_h, r1_h, act_h, dg_h, z2_h, r2_h,
    wq_h, wk_h, wv_h, wo_h, wi_h, w2_h,
    lse, seg_row, seg_col, dpool, g1, g2,
    tok_o, douter_o, dinner_o, dout_o, dq_o, dk_o, dv_o, vec_o,
    grads, *rest,
):
    S = len(dims)
    land, rest = rest[:S], rest[S:]
    (
        b0, b1, b2, b3, b4, b5, b6, b7, b8, b9, b10, grad, rbuf, bias, vbuf, vrecv,
        lsem, ssem, rsem, osem, vs, vr, freed, slot, tsem,
    ) = rest
    total, width = grads.shape
    rows = x_h.shape[0]
    nrow = seg_row.shape[0]
    seqlen = rows // nrow
    pairs = width // 128
    nff = w2_h.shape[0] // width
    TM = 256
    CH = 8 << S
    C = total // CH
    NS = land[0].shape[0] // (CH // 2)
    M = CH // UNIT
    route = Route(dims)
    bar = pltpu.get_barrier_semaphore()

    def plain(k):
        axis, bit = dims[k]
        where = list(route.pos)
        where[axis] = where[axis] + bit * (1 - 2 * route.bits[k])
        return tuple(where)

    for k in range(S):
        pl.semaphore_signal(bar, inc=1, device_id=plain(k), device_id_type=MESH)

    def tile(i, size=TM):
        return pl.ds(pl.multiple_of(i * size, size), size)

    square = pl.ds(0, width)

    def load(i, src, dst):
        return pltpu.make_async_copy(src, dst, lsem.at[i])

    def columns(j):
        return pl.ds(pl.multiple_of(j * width, width), width)

    def l_act(j):
        return load(j, act_h.at[:, columns(j)], b0)

    def l_dg(j):
        return load(nff + j, dg_h.at[:, columns(j)], b1)

    def l_w2(j):
        return load(2 * nff + j, w2_h.at[columns(j)], b2.at[square])

    def l_wi(j):
        return load(3 * nff + j, wi_h.at[:, columns(j)], b3.at[square])

    n = 4 * nff
    l_cot = load(n, cot_h, b7)
    l_z2 = load(n + 1, z2_h, b8)
    l_r2 = load(n + 2, r2_h, rbuf)
    l_nb = load(n + 3, nb_h, b5)
    l_q = load(n + 4, q_h, b7)
    l_k = load(n + 5, k_h, b8)
    l_v = load(n + 6, v_h, b9)
    l_wo = load(n + 7, wo_h, b10.at[square])
    l_r1 = load(n + 8, r1_h, rbuf)
    l_z1 = load(n + 9, z1_h, b0)
    l_c = load(n + 10, c_h, b6)
    l_x = load(n + 11, x_h, b5)
    l_wq = load(n + 12, wq_h, b7.at[square])
    l_wk = load(n + 13, wk_h, b8.at[square])
    l_wv = load(n + 14, wv_h, b9.at[square])

    for c in (l_cot, l_z2, l_r2, l_act(0), l_w2(0), l_dg(0), l_nb, l_wi(0), l_v, l_wo):
        c.start()

    DQB, DVB, DOB, DNG, DNS, DIB = 0, 1, 2, 3, 4, 5
    D2B, DFG, DFS = DIB + nff, DIB + nff + 1, DIB + nff + 2
    vbuf[...] = jnp.zeros_like(vbuf)

    def vadd(i, value):
        vbuf[0, pl.ds(i, 1)] = vbuf[0, pl.ds(i, 1)] + value

    def second():
        kinds = lax.broadcasted_iota(jnp.int32, (S_ROW, seqlen), 0)
        for r in range(nrow):
            onehot = (seg_row[r] == kinds).astype(F32)
            count = jnp.sum(onehot, axis=1, keepdims=True)
            share = dpool[r * S_ROW : (r + 1) * S_ROW] / count
            grad[pl.ds(r * seqlen, seqlen)] = dot(onehot, share, 0, 0, HIGH)
        l_cot.wait()
        l_z2.wait()
        l_r2.wait()

        def body(i, _):
            dx = b7[tile(i)].astype(F32) + grad[tile(i)]
            dh, dg, db = norm_grad(dx, b8[tile(i)].astype(F32), rbuf[tile(i), 0:1], g2[...])
            grad[tile(i)] = dh
            b4[tile(i)] = dh.astype(BF)
            vadd(DFG, dg)
            vadd(DFS, db)
            vadd(D2B, jnp.sum(dh, axis=0, keepdims=True))
            return 0

        lax.fori_loop(0, rows // TM, body, 0)
        l_q.start()
        l_k.start()
        l_r1.start()

    def outer(left, right, block):
        def body(i, _):
            cols = pl.ds(pl.multiple_of(i * TM, TM), TM)
            at = pl.multiple_of(block * width + i * TM, TM)
            grads[pl.ds(at, TM)] = dot(left[:, cols], right[...], 0, 0)
            return 0

        lax.fori_loop(0, width // TM, body, 0)

    def ffn_outer(j):
        l_act(j).wait()
        outer(b0, b4, 2 * j)

        @pl.when(j < nff - 1)
        def _():
            l_act(j + 1).start()

        @pl.when(j == nff - 1)
        def _():
            l_z1.start()

    def ffn_inner(j):
        l_w2(j).wait()
        l_dg(j).wait()

        def body(i, _):
            gi = dot(b4[tile(i)], b2[square], 1, 1) * b1[tile(i)].astype(F32)
            b6[tile(i)] = gi.astype(BF)
            vadd(DIB + j, jnp.sum(gi, axis=0, keepdims=True))
            return 0

        lax.fori_loop(0, rows // TM, body, 0)

        @pl.when(j < nff - 1)
        def _():
            l_w2(j + 1).start()
            l_dg(j + 1).start()

    def ffn_dinner(j):
        @pl.when(j == 0)
        def _():
            l_nb.wait()

        outer(b5, b6, 2 * j + 1)

        @pl.when(j == nff - 1)
        def _():
            l_x.start()

    def ffn_back(j):
        l_wi(j).wait()

        def body(i, _):
            grad[tile(i)] = grad[tile(i)] + dot(b6[tile(i)], b3[square], 1, 1)
            return 0

        lax.fori_loop(0, rows // TM, body, 0)

        @pl.when(j < nff - 1)
        def _():
            l_wi(j + 1).start()

        @pl.when(j == nff - 1)
        def _():
            l_c.start()

    def first():
        l_z1.wait()
        l_r1.wait()

        def body(i, _):
            dh, dg, db = norm_grad(grad[tile(i)], b0[tile(i)].astype(F32), rbuf[tile(i), 0:1], g1[...])
            grad[tile(i)] = dh
            b4[tile(i)] = dh.astype(BF)
            vadd(DNG, dg)
            vadd(DNS, db)
            vadd(DOB, jnp.sum(dh, axis=0, keepdims=True))
            return 0

        lax.fori_loop(0, rows // TM, body, 0)

    def project():
        l_c.wait()
        l_wo.wait()
        outer(b6, b4, 2 * nff)

        def body(i, _):
            b3[tile(i)] = dot(b4[tile(i)], b10[square], 1, 1).astype(BF)
            return 0

        lax.fori_loop(0, rows // TM, body, 0)
        l_q.wait()
        l_k.wait()
        l_v.wait()

    parts = halves()

    def attention(a):
        r = a // (pairs // 2)
        span = tile(r, seqlen)
        bias[...] = jnp.where(seg_col[span] == seg_row[r], 0.0, masked_score).astype(F32)

        def pair(i, _):
            p = (a - r * (pairs // 2)) * 2 + i
            lanes = pl.ds(pl.multiple_of(p * 128, 128), 128)
            qp = b7[span, lanes] * jnp.asarray(0.125, BF)
            kp = b8[span, lanes]
            vp = b9[span, lanes]
            dc = b3[span, lanes]
            dq = dk = dv = 0.0
            for half, part in enumerate(parts):
                k1 = kp * part
                s = dot(k1, qp, 1, 1) + bias[...]
                prob = jnp.exp(s - lse[(r * pairs + p) * 2 + half])
                dp = dot(vp * part, dc, 1, 1)
                dv = dv + dot(prob.astype(BF), dc * part, 1, 0)
                mean = jnp.sum(prob * dp, axis=0, keepdims=True)
                ds = (prob * (dp - mean)).astype(BF)
                dk = dk + dot(ds, qp * part, 1, 0)
                dq = dq + dot(k1, ds, 0, 0)
            dq = 0.125 * dq.T
            b0[span, lanes] = dq.astype(BF)
            b1[span, lanes] = dk.astype(BF)
            b2[span, lanes] = dv.astype(BF)
            vbuf[0, DQB : DQB + 1, lanes] = vbuf[0, DQB : DQB + 1, lanes] + jnp.sum(dq, axis=0, keepdims=True)
            vbuf[0, DVB : DVB + 1, lanes] = vbuf[0, DVB : DVB + 1, lanes] + jnp.sum(dv, axis=0, keepdims=True)
            return 0

        lax.fori_loop(0, 2, pair, 0)

    def token_part(i):
        out = grad[tile(i)] + dot(b0[tile(i)], b7[square], 1, 1)
        out = out + dot(b1[tile(i)], b8[square], 1, 1)
        grad[tile(i)] = out + dot(b2[tile(i)], b9[square], 1, 1)

    T_LN = 4 * nff - 1
    A0 = T_LN + 2
    A1 = A0 + nrow * pairs // 2
    T_TOK = A1 + 3
    T_END = T_TOK + rows // TM

    def slices(t):
        u = t + 1
        j = u // 4

        for kind, work in enumerate((ffn_outer, ffn_inner, ffn_dinner, ffn_back)):
            @pl.when((u < 4 * nff) & (u - 4 * j == kind))
            def _():
                work(j)

        pl.when(t == T_LN)(first)
        pl.when(t == T_LN + 1)(project)

        @pl.when((t >= A0) & (t < A1))
        def _():
            attention(t - A0)

        @pl.when(t == A1)
        def _():
            l_wq.start()
            l_wk.start()
            l_wv.start()
            l_x.wait()

        for i, src in enumerate((b0, b1, b2)):
            @pl.when(t == A1 + i)
            def _():
                outer(b5, src, 2 * nff + 1 + i)

        @pl.when(t == T_TOK)
        def _():
            l_wq.wait()
            l_wk.wait()
            l_wv.wait()

        @pl.when((t >= T_TOK) & (t < T_END))
        def _():
            token_part(t - T_TOK)

        @pl.when(t == T_END)
        def _():
            pltpu.make_async_copy(grad, tok_o, tsem).start()

    def offset(s, c):
        o = c * CH
        for k in range(s):
            o = o + route.bit(k, colour_of(c)) * (CH >> (k + 1))
        return o

    def reduce_copy(s, c):
        half = CH >> (s + 1)
        b = route.bit(s, colour_of(c))
        o = offset(s, c)
        keep = pl.multiple_of(o + b * half, 8)
        send = pl.multiple_of(o + (1 - b) * half, 8)
        here = pl.multiple_of((c % NS) * half, 8)
        cp = pltpu.make_async_remote_copy(
            grads.at[pl.ds(send, half)], land[s].at[pl.ds(here, half)],
            ssem.at[s, c], rsem.at[s, c],
            device_id=route.partner(s, colour_of(c)), device_id_type=MESH,
        )
        return cp, keep, here, half

    def gather_copy(s, c):
        half = CH >> (s + 1)
        keep = pl.multiple_of(offset(s, c) + route.bit(s, colour_of(c)) * half, 8)
        rank = 2 * S - 1 - s
        return pltpu.make_async_remote_copy(
            grads.at[pl.ds(keep, half)], grads.at[pl.ds(keep, half)],
            ssem.at[rank, c], rsem.at[rank, c],
            device_id=route.partner(s, colour_of(c)), device_id_type=MESH,
        )

    per = width // UNIT

    def out_copies(c, start):
        for i in range(M):
            unit = c * M + i
            src = grads.at[pl.ds(pl.multiple_of(unit * UNIT, UNIT), UNIT)]
            if not start:
                pltpu.make_async_copy(src, dq_o.at[pl.ds(0, UNIT)], osem.at[unit]).wait()
                continue
            block = unit // per
            line = pl.multiple_of((unit - block * per) * UNIT, UNIT)
            for b in range(2 * nff + 4):
                if b >= 2 * nff:
                    dst = (dout_o, dq_o, dk_o, dv_o)[b - 2 * nff].at[pl.ds(line, UNIT)]
                elif b % 2 == 0:
                    dst = douter_o.at[pl.ds(b // 2 * width + line, UNIT)]
                else:
                    dst = dinner_o.at[pl.ds(line, UNIT), pl.ds(b // 2 * width, width)]

                @pl.when(block == b)
                def _():
                    pltpu.make_async_copy(src, dst, osem.at[unit]).start()

    def start(p, c):
        if p < S:
            @pl.when(c >= NS)
            def _():
                pl.semaphore_wait(slot.at[p, c], 1)

            reduce_copy(p, c)[0].start()
        elif p < 2 * S:
            s = 2 * S - 1 - p
            pl.semaphore_wait(freed.at[s, c], 1)
            gather_copy(s, c).start()
        else:
            out_copies(c, True)

    def finish(p, c):
        if p < S:
            cp, keep, here, half = reduce_copy(p, c)
            cp.wait_recv()
            grads[pl.ds(keep, half)] = grads[pl.ds(keep, half)] + land[p][pl.ds(here, half)]
            cp.wait_send()
            pl.semaphore_signal(
                freed.at[p, c], inc=1, device_id=route.partner(p, colour_of(c)), device_id_type=MESH
            )

            @pl.when(c + NS < C)
            def _():
                pl.semaphore_signal(
                    slot.at[p, c + NS], inc=1,
                    device_id=route.partner(p, colour_of(c + NS)), device_id_type=MESH,
                )
        elif p < 2 * S:
            gather_copy(2 * S - 1 - p, c).wait()
        else:
            out_copies(c, False)

    def vec_copy(r):
        return pltpu.make_async_remote_copy(
            vbuf.at[r], vrecv.at[r], vs.at[r], vr.at[r], device_id=plain(r), device_id_type=MESH
        )

    NP = 2 * S + 1

    def at(t, p):
        if M == 1:
            c = t - 2 * p
            return c, (c >= 0) & (c < C)
        c = (t - 2 * p + 1) // M - 1
        return c, (c >= 0) & (c < C) & ((c + 1) * M == t - 2 * p + 1)

    def step(t, _):
        for p in range(NP):
            c, valid = at(t, p)
            pl.when(valid)(functools.partial(start, p, c))
        for r in range(S):
            @pl.when(t == T_TOK + 2 * r)
            def _():
                vec_copy(r).start()
        slices(t)
        for p in range(NP):
            c, valid = at(t - 1, p)
            pl.when(valid)(functools.partial(finish, p, c))
        for r in range(S):
            @pl.when(t == T_TOK + 1 + 2 * r)
            def _():
                cp = vec_copy(r)
                cp.wait()
                vbuf[r + 1] = vbuf[r] + vrecv[r]
        return 0

    second()
    ffn_outer(0)
    pl.semaphore_wait(bar, S)
    steps = max(C * M + 2 * (NP - 1) + 1, T_TOK + 2 * S, T_END + 1)
    lax.fori_loop(0, steps, step, 0)
    pltpu.make_async_copy(grad, tok_o, tsem).wait()
    vec_o[...] = vbuf[S]


def backward_reduce(
    tokens, cotangent, kept, weights, lse, segment, dpooled, g1, g2, dp_size, bucket_size
):
    rows, width = tokens.shape
    nrow, seqlen = segment.shape
    wq, wk, wv, wo, wi, w2 = weights
    inner = wi.shape[1]
    nff = inner // width
    dims = bit_dims(dp_size, bucket_size)
    S = len(dims)
    CH = 8 << S
    total = (2 * nff + 4) * width
    C = total // CH
    NS = max(2, 2048 // CH)
    nvec = -(-(8 + nff) // 8) * 8
    vm = pl.BlockSpec(memory_space=pltpu.VMEM)
    hbm = pl.BlockSpec(memory_space=pl.ANY)
    sd = jax.ShapeDtypeStruct
    dma = pltpu.SemaphoreType.DMA
    plain = pltpu.SemaphoreType.REGULAR
    full = sd((width, width), F32)
    row = lambda a: a.reshape(1, -1)
    return pl.pallas_call(
        functools.partial(backward_kernel, dims),
        name="backward_reduce",
        out_shape=(
            sd((rows, width), F32), sd((inner, width), F32), sd((width, inner), F32),
            full, full, full, full, sd((nvec, width), F32),
        ),
        in_specs=[hbm] * 19 + [vm] * 6,
        out_specs=[hbm] * 7 + [vm],
        scratch_shapes=[pltpu.VMEM((total, width), F32)]
        + [pltpu.VMEM((NS * (CH >> (s + 1)), width), F32) for s in range(S)]
        + [pltpu.VMEM((rows, width), BF)] * 11
        + [
            pltpu.VMEM((rows, width), F32), pltpu.VMEM((rows, 128), F32),
            pltpu.VMEM((seqlen, seqlen), F32), pltpu.VMEM((S + 1, nvec, width), F32),
            pltpu.VMEM((S, nvec, width), F32),
            dma((4 * nff + 15,)), dma((2 * S, C)), dma((2 * S, C)), dma((total // UNIT,)),
            dma((S,)), dma((S,)), plain((S, C)), plain((S, C)), dma,
        ],
        compiler_params=pltpu.CompilerParams(
            collective_id=1, has_side_effects=True, vmem_limit_bytes=67043328
        ),
    )(
        tokens, cotangent, *kept, wq, wk, wv, wo, wi, w2, lse,
        segment.reshape(nrow, 1, seqlen), segment.reshape(rows, 1), dpooled, row(g1), row(g2),
    )


def local(
    dp_size, bucket_size,
    tokens, segment, pair_order, cotangent, query_weight, query_bias, key_weight, value_weight,
    value_bias, out_weight, out_bias, norm_gain, norm_shift, inner_weight, inner_bias,
    outer_weight, outer_bias, final_gain, final_shift,
):
    width = tokens.shape[1]
    (
        query_b, key_b, value_b, context_b, normed_b, z1, r1, active_b, slope, z2, r2, lse,
        layer_out, pooled,
    ) = forward(
        tokens, segment, query_weight, query_bias, key_weight, value_weight, value_bias,
        out_weight, out_bias, norm_gain, norm_shift, inner_weight, inner_bias, outer_weight,
        outer_bias, final_gain, final_shift,
    )
    dpooled, loss_value = pair_loss(pooled, pair_order, dp_size, bucket_size)
    loss_value = loss_value.reshape(())
    kept = (
        query_b, key_b, value_b, context_b, normed_b, z1, r1, active_b, slope, z2, r2,
    )
    weights = (query_weight, key_weight, value_weight, out_weight, inner_weight, outer_weight)
    (
        tokens_grad, douter_weight, dinner_weight, dout_weight, dquery_weight, dkey_weight,
        dvalue_weight, packed,
    ) = backward_reduce(
        tokens, cotangent, kept, weights, lse, segment, dpooled, norm_gain, final_gain,
        dp_size, bucket_size,
    )
    packed = packed.reshape(-1)
    sizes = [width] * 5 + [inner_bias.shape[0]] + [width] * 3
    ends = [sum(sizes[: i + 1]) for i in range(len(sizes))]
    (
        dquery_bias, dvalue_bias, dout_bias, dnorm_gain, dnorm_shift,
        dinner_bias, douter_bias, dfinal_gain, dfinal_shift,
    ) = (packed[e - n : e] for e, n in zip(ends, sizes))
    return (
        layer_out, loss_value, tokens_grad, dquery_weight, dquery_bias, dkey_weight,
        dvalue_weight, dvalue_bias, dout_weight, dout_bias, dnorm_gain, dnorm_shift,
        dinner_weight, dinner_bias, douter_weight, douter_bias, dfinal_gain, dfinal_shift,
    )


def solution(mesh):
    split = P(("dp", "bucket"), None)
    return jax.shard_map(
        functools.partial(local, mesh.shape["dp"], mesh.shape["bucket"]),
        mesh=mesh,
        in_specs=(split, split, P(), split) + (P(),) * 15,
        out_specs=(split, P(), split) + (P(),) * 15,
        check_vma=False,
    )
```

```python
import functools

import jax
import jax.numpy as jnp
import numpy as np
from jax import lax
from jax.experimental import pallas as pl
from jax.experimental.pallas import tpu as pltpu
from jax.sharding import PartitionSpec as P

S_ROW = 8
norm_eps = 1e-05
masked_score = -1000000000.0
BF = jnp.bfloat16
F32 = jnp.float32
HIGH = lax.Precision.HIGHEST


def dot(a, b, da, db, precision=None):
    return lax.dot_general(
        a, b, (((da,), (db,)), ((), ())), precision=precision, preferred_element_type=F32
    )


def halves(width=128):
    lane = lax.broadcasted_iota(jnp.int32, (1, width), 1)
    low = (lane < width // 2).astype(F32)
    return low.astype(BF), (1.0 - low).astype(BF)


def column(line):
    tall = jnp.broadcast_to(line.astype(F32), (8, line.shape[1])).T
    return tall[:, :1].astype(jnp.int32)


def normalise(hidden):
    centred = hidden - jnp.mean(hidden, axis=-1, keepdims=True)
    rate = lax.rsqrt(jnp.mean(centred * centred, axis=-1, keepdims=True) + norm_eps)
    return centred * rate, rate


def forward_kernel(
    x_in, seg, wq_h, bq, wk_h, wv_h, bv, wo_h, bo, g1, s1, wi_h, bi, w2_h, b2, g2, s2,
    q_o, k_o, v_o, c_o, nb_o, z1_o, r1_o, act_o, dg_o, z2_o, r2_o, lse_o, out_o, pool_o,
    wq, wk, wv, wo, wi, w2, q, k, v, ctx, nf, nb, z1, r1, act, dg, z2, r2, fin, lout, bias, flat,
    wsem, osem,
):
    rows, width = x_in.shape
    nrow = seg.shape[0]
    seqlen = rows // nrow
    pairs = width // 128
    inner = wi.shape[1]
    TM = 256
    loads = [
        pltpu.make_async_copy(a, b, wsem.at[i])
        for i, (a, b) in enumerate(
            [(wq_h, wq), (wk_h, wk), (wv_h, wv), (wo_h, wo), (wi_h, wi), (w2_h, w2)]
        )
    ]
    for c in loads:
        c.start()
    row_refs = []
    for i, a in enumerate((bq, bv, bo, g1, s1, b2, g2, s2)):
        at = flat.at[pl.ds(i, 1), pl.ds(0, width)]
        at[...] = a[...].reshape(1, -1)
        row_refs.append(at)
    bq, bv, bo, g1, s1, b2, g2, s2 = row_refs
    flat[8:9] = bi[...].reshape(1, -1)
    stores = []

    def put(i, src, dst):
        c = pltpu.make_async_copy(src, dst, osem.at[i])
        c.start()
        stores.append(c)

    def tile(i):
        return pl.ds(pl.multiple_of(i * TM, TM), TM)

    for c in loads[:3]:
        c.wait()

    def project(i, _):
        x = x_in[tile(i)]
        q[tile(i)] = (dot(x, wq[...], 1, 0) + bq[...]).astype(BF)
        k[tile(i)] = dot(x, wk[...], 1, 0).astype(BF)
        v[tile(i)] = (dot(x, wv[...], 1, 0) + bv[...]).astype(BF)
        return 0

    lax.fori_loop(0, rows // TM, project, 0)
    put(0, q, q_o)
    put(1, k, k_o)
    put(2, v, v_o)
    parts = halves()

    def row(r, _):
        span = pl.ds(pl.multiple_of(r * seqlen, seqlen), seqlen)
        line = seg[pl.ds(r, 1)]
        same = column(line) == line
        bias[...] = jnp.where(same, 0.0, masked_score).astype(F32)

        def pair(p, _):
            lanes = pl.ds(pl.multiple_of(p * 128, 128), 128)
            qp = q[span, lanes] * jnp.asarray(0.125, BF)
            kp = k[span, lanes]
            vp = v[span, lanes]
            total = None
            for half, part in enumerate(parts):
                s = dot(kp * part, qp, 1, 1) + bias[...]
                top = jnp.max(s, axis=0, keepdims=True)
                e = jnp.exp(s - top)
                mass = jnp.sum(e, axis=0, keepdims=True)
                prob = (e * (1.0 / mass)).astype(BF)
                c = dot(vp * part, prob, 0, 0)
                total = c if total is None else total + c
                lse_o[r * pairs * 2 + p * 2 + half] = top + jnp.log(mass)
            ctx[span, lanes] = total.T.astype(BF)
            return 0

        lax.fori_loop(0, pairs, pair, 0)
        return 0

    lax.fori_loop(0, nrow, row, 0)
    put(3, ctx, c_o)
    loads[3].wait()

    def attend(i, _):
        first = x_in[tile(i)].astype(F32) + dot(ctx[tile(i)], wo[...], 1, 0) + bo[...]
        z, rate = normalise(first)
        normed = z * g1[...] + s1[...]
        nf[tile(i)] = normed
        nb[tile(i)] = normed.astype(BF)
        z1[tile(i)] = z.astype(BF)
        r1[tile(i)] = jnp.broadcast_to(rate, (TM, 128))
        return 0

    lax.fori_loop(0, rows // TM, attend, 0)
    put(4, nb, nb_o)
    put(5, z1, z1_o)
    put(6, r1, r1_o)
    loads[4].wait()
    loads[5].wait()
    TF = 512

    def feed(i, _):
        def block(j, _):
            cols = pl.ds(pl.multiple_of(j * TF, TF), TF)
            h = dot(nb[tile(i)], wi[:, cols], 1, 0) + flat[8:9, cols]
            cdf = 0.5 + 0.5 * lax.erf(h * 0.7071067811865476)
            act_b = (h * cdf).astype(BF)
            act[tile(i), cols] = act_b
            slope = cdf + h * (0.3989422804014327 * jnp.exp(-0.5 * h * h))
            dg[tile(i), cols] = slope.astype(BF)
            return 0

        lax.fori_loop(0, inner // TF, block, 0)
        second = nf[tile(i)] + dot(act[tile(i)], w2[...], 1, 0) + b2[...]
        z, rate = normalise(second)
        final = z * g2[...] + s2[...]
        fin[tile(i)] = final
        lout[tile(i)] = final.astype(BF)
        z2[tile(i)] = z.astype(BF)
        r2[tile(i)] = jnp.broadcast_to(rate, (TM, 128))
        return 0

    lax.fori_loop(0, rows // TM, feed, 0)
    put(7, act, act_o)
    put(8, dg, dg_o)
    put(9, z2, z2_o)
    put(10, r2, r2_o)
    put(11, lout, out_o)
    for r in range(nrow):
        kinds = lax.broadcasted_iota(jnp.int32, (S_ROW, seqlen), 0)
        onehot = (seg[r : r + 1] == kinds).astype(F32)
        count = jnp.sum(onehot, axis=1, keepdims=True)
        got = dot(onehot, fin[r * seqlen : (r + 1) * seqlen], 1, 0, HIGH)
        pool_o[r * S_ROW : (r + 1) * S_ROW] = got / count
    for c in stores:
        c.wait()


def forward(tokens, segment, wq, bq, wk, wv, bv, wo, bo, g1, s1, wi, bi, w2, b2, g2, s2):
    rows, width = tokens.shape
    nrow, seqlen = segment.shape
    inner = wi.shape[1]
    heads = width // 64
    vm = pl.BlockSpec(memory_space=pltpu.VMEM)
    hbm = pl.BlockSpec(memory_space=pl.ANY)
    act = (rows, width)
    wide = (rows, inner)
    sd = jax.ShapeDtypeStruct
    outs = (
        sd(act, BF), sd(act, BF), sd(act, BF), sd(act, BF), sd(act, BF), sd(act, BF),
        sd((rows, 128), F32), sd(wide, BF), sd(wide, BF), sd(act, BF), sd((rows, 128), F32),
        sd((nrow * heads, 1, seqlen), F32), sd(act, BF), sd((nrow * S_ROW, width), F32),
    )
    return pl.pallas_call(
        forward_kernel,
        name="forward",
        out_shape=outs,
        in_specs=[vm, vm, hbm, vm, hbm, hbm, vm, hbm, vm, vm, vm, hbm, vm, hbm, vm, vm, vm],
        out_specs=[hbm] * 11 + [vm, hbm, vm],
        scratch_shapes=[pltpu.VMEM((width, width), BF)] * 4
        + [pltpu.VMEM((width, inner), BF), pltpu.VMEM((inner, width), BF)]
        + [pltpu.VMEM(act, BF)] * 4
        + [pltpu.VMEM(act, F32), pltpu.VMEM(act, BF), pltpu.VMEM(act, BF), pltpu.VMEM((rows, 128), F32)]
        + [pltpu.VMEM(wide, BF), pltpu.VMEM(wide, BF), pltpu.VMEM(act, BF), pltpu.VMEM((rows, 128), F32)]
        + [pltpu.VMEM(act, F32), pltpu.VMEM(act, BF), pltpu.VMEM((seqlen, seqlen), F32)]
        + [pltpu.VMEM((16, inner), F32)]
        + [pltpu.SemaphoreType.DMA((6,)), pltpu.SemaphoreType.DMA((12,))],
        compiler_params=pltpu.CompilerParams(vmem_limit_bytes=64000000),
    )(
        tokens, segment, wq, bq, wk, wv, bv, wo, bo, g1, s1, wi, bi, w2, b2, g2, s2,
    )


MESH = pl.DeviceIdType.MESH

def bit_dims(dp_size, bucket_size):
    dims = []
    for axis, size in ((1, bucket_size), (0, dp_size)):
        bit = 1
        while bit < size:
            dims.append((axis, bit))
            bit *= 2
    return dims

class Route:
    def __init__(self, dims):
        self.dims = dims
        self.pos = (lax.axis_index("dp"), lax.axis_index("bucket"))
        self.bits = [(self.pos[a] // b) % 2 for a, b in dims]

    def weights(self, stage, colour=0):
        n = len(self.dims)
        if stage == 0 or n < 3:
            return {stage: 1}
        order = list(range(n))
        if colour:
            order = [0] + order[3:] + [1, 2]
        d = order[stage]
        if d in (1, 2):
            core = self.bits[0]
            return {d: 1 - core, 3 - d: core}
        return {d: 1}

    def bit(self, stage, colour=0):
        w = self.weights(stage, colour)
        return sum(v * self.bits[k] for k, v in w.items())

    def partner(self, stage, colour=0):
        where = list(self.pos)
        for k, v in self.weights(stage, colour).items():
            axis, bit = self.dims[k]
            where[axis] = where[axis] + v * (bit * (1 - 2 * self.bits[k]))
        return tuple(where)


cos_scale = 20.0


def gather_order(dims, dp_size, bucket_size, own):
    S = len(dims)
    n = np.arange(dp_size * bucket_size)
    key = [(n >> (S - 1 - s)) & 1 for s in range(S)]
    if S >= 3:
        core = key[0]
        key[1], key[2] = np.where(core == 1, key[2], key[1]), np.where(core == 1, key[1], key[2])
    pos = [0, 0]
    for (axis, bit), value in zip(dims, key):
        pos[axis] = pos[axis] + bit * value
    device = pos[0] * bucket_size + pos[1]
    return (device[:, None] * own + np.arange(own)[None, :]).reshape(1, -1).astype(np.int32)


def sphere(vectors):
    factor = lax.rsqrt(jnp.sum(vectors * vectors, axis=1, keepdims=True) + 1e-06)
    return vectors * factor, factor


def loss_kernel(dims, bucket_size, pool, sid, order, dpool, loss, buf, unit, weigh, tall, ssem, rsem):
    own, width = pool.shape
    sents = buf.shape[0]
    pairs = sents // 2
    S = len(dims)
    route = Route(dims)
    pair_row = order[...].reshape(1, -1)
    tall[...] = jnp.broadcast_to(column(pair_row), tall.shape)
    bar = pltpu.get_barrier_semaphore()
    for k in range(S):
        axis, bit = dims[k]
        where = list(route.pos)
        where[axis] = where[axis] + bit * (1 - 2 * route.bits[k])
        pl.semaphore_signal(bar, inc=1, device_id=tuple(where), device_id_type=MESH)
    base = [0]
    for s in range(S):
        base.append(base[s] + route.bit(s) * (sents >> (s + 1)))
    buf[pl.ds(pl.multiple_of(base[S], 8), own)] = pool[...]
    pl.semaphore_wait(bar, S)
    for s in reversed(range(S)):
        half = sents >> (s + 1)
        here = pl.ds(pl.multiple_of(base[s + 1], 8), half)
        c = pltpu.make_async_remote_copy(
            buf.at[here], buf.at[here], ssem.at[s], rsem.at[s],
            device_id=route.partner(s), device_id_type=MESH,
        )
        c.start()
        c.wait()
    B = min(256, pairs)
    for i in range(sents // B):
        part = pl.ds(i * B, B)
        pick = (tall[part, 0:1] == sid[...]).astype(F32)
        ordered = dot(pick, buf[...], 1, 0, HIGH)
        unit[part] = sphere(ordered)[0]
    total = jnp.zeros((1, 1), F32)
    for i in range(pairs // B):
        part = pl.ds(i * B, B)
        logits = cos_scale * dot(unit[part], unit[pairs:], 1, 1, HIGH)
        top = jnp.max(logits, axis=1, keepdims=True)
        row_lse = top + jnp.log(jnp.sum(jnp.exp(logits - top), axis=1, keepdims=True))
        line = lax.broadcasted_iota(jnp.int32, logits.shape, 0) + i * B
        eye = (line == lax.broadcasted_iota(jnp.int32, logits.shape, 1)).astype(F32)
        weigh[part] = jnp.exp(logits - row_lse) - eye
        gap = row_lse - jnp.sum(logits * eye, axis=1, keepdims=True)
        total = total + jnp.sum(gap, axis=0, keepdims=True)
    loss[...] = total
    first = (route.pos[0] * bucket_size + route.pos[1]) * own
    mine = lax.broadcasted_iota(jnp.int32, (own, sents), 0) + first
    choose = (mine == pair_row).astype(F32)
    by_row = dot(choose[:, :pairs], weigh[...], 1, 0, HIGH)
    by_column = dot(choose[:, pairs:], weigh[...], 1, 1, HIGH)
    grad = cos_scale * (dot(by_row, unit[pairs:], 1, 0, HIGH) + dot(by_column, unit[:pairs], 1, 0, HIGH))
    u, factor = sphere(pool[...])
    dpool[...] = factor * (grad - u * jnp.sum(u * grad, axis=1, keepdims=True))


def pair_loss(pool, pair_order, dp_size, bucket_size):
    dims = bit_dims(dp_size, bucket_size)
    S = len(dims)
    own, width = pool.shape
    sents = pair_order.shape[0]
    vm = pl.BlockSpec(memory_space=pltpu.VMEM)
    sid = jnp.asarray(gather_order(dims, dp_size, bucket_size, own))
    return pl.pallas_call(
        functools.partial(loss_kernel, dims, bucket_size),
        name="pair_loss",
        out_shape=(jax.ShapeDtypeStruct(pool.shape, F32), jax.ShapeDtypeStruct((1, 1), F32)),
        in_specs=[vm] * 3, out_specs=(vm, vm),
        scratch_shapes=[
            pltpu.VMEM((sents, width), F32), pltpu.VMEM((sents, width), F32),
            pltpu.VMEM((sents // 2, sents // 2), F32), pltpu.VMEM((sents, 128), jnp.int32),
            pltpu.SemaphoreType.DMA((S,)), pltpu.SemaphoreType.DMA((S,)),
        ],
        compiler_params=pltpu.CompilerParams(collective_id=2, has_side_effects=True, vmem_limit_bytes=60000000),
    )(pool, sid, pair_order)


NARROW = 128
VMEM_KERNEL = 33800000
LAG = 2
FIN = 1


def norm_grad(dx, z, rate, gain):
    dz = dx * gain
    mean = jnp.mean(dz, axis=-1, keepdims=True)
    cross = jnp.mean(dz * z, axis=-1, keepdims=True)
    dh = rate * (dz - mean - z * cross)
    return dh, jnp.sum(dx * z, axis=0, keepdims=True), jnp.sum(dx, axis=0, keepdims=True)


def backward_kernel(
    dims,
    x_h, cot_h, q_h, k_h, v_h, c_h, nb_h, z1_h, r1_h, act_h, dg_h, z2_h, r2_h,
    wq_h, wk_h, wv_h, wo_h, wi_h, w2_h,
    lse, seg, dpool, g1_in, g2_in,
    grads, grad, vec_o,
    *rest,
):
    S = len(dims)
    land, rest = rest[:S], rest[S:]
    (
        b0, b1, b2, b3, b4, b5, b6, b7, b8, b9, b10, rbuf, bias, gains, vbuf, vrecv,
        lsem, ssem, rsem, vs, vr, freed, slot,
    ) = rest
    total, width = grads.shape
    rows = x_h.shape[0]
    nrow = seg.shape[0]
    seqlen = rows // nrow
    pairs = width // 128
    nff = w2_h.shape[0] // width
    TM = 256
    CH = 8 << S
    C = total // CH
    NS = land[0].shape[0] // (CH // 2)
    M = CH // 256
    route = Route(dims)
    bar = pltpu.get_barrier_semaphore()

    def plain(k):
        axis, bit = dims[k]
        where = list(route.pos)
        where[axis] = where[axis] + bit * (1 - 2 * route.bits[k])
        return tuple(where)

    for k in range(S):
        pl.semaphore_signal(bar, inc=1, device_id=plain(k), device_id_type=MESH)

    def tile(i, size=TM):
        return pl.ds(pl.multiple_of(i * size, size), size)

    square = pl.ds(0, width)

    def load(i, src, dst):
        return pltpu.make_async_copy(src, dst, lsem.at[i])

    def columns(j):
        return pl.ds(pl.multiple_of(j * width, width), width)

    def l_act(j):
        return load(j, act_h.at[:, columns(j)], b0)

    def l_dg(j):
        return load(nff + j, dg_h.at[:, columns(j)], b1)

    def l_w2(j):
        return load(2 * nff + j, w2_h.at[columns(j)], b2.at[square])

    def l_wi(j):
        return load(3 * nff + j, wi_h.at[:, columns(j)], b3.at[square])

    n = 4 * nff
    l_cot = load(n, cot_h, b7)
    l_z2 = load(n + 1, z2_h, b8)
    l_r2 = load(n + 2, r2_h, rbuf)
    l_nb = load(n + 3, nb_h, b5)
    l_q = load(n + 4, q_h, b7)
    l_k = load(n + 5, k_h, b8)
    l_v = load(n + 6, v_h, b9)
    l_wo = load(n + 7, wo_h, b10.at[square])
    l_r1 = load(n + 8, r1_h, rbuf)
    l_z1 = load(n + 9, z1_h, b0)
    l_c = load(n + 10, c_h, b6)
    l_x = load(n + 11, x_h, b5)
    l_wq = load(n + 12, wq_h, b7.at[square])
    l_wk = load(n + 13, wk_h, b8.at[square])
    l_wv = load(n + 14, wv_h, b9.at[square])

    for c in (l_cot, l_z2, l_r2, l_act(0), l_w2(0), l_dg(0), l_nb, l_wi(0), l_v, l_wo):
        c.start()

    DQB, DVB, DOB, DNG, DNS, DIB = 0, 1, 2, 3, 4, 5
    D2B, DFG, DFS = DIB + nff, DIB + nff + 1, DIB + nff + 2
    vbuf[...] = jnp.zeros_like(vbuf)
    g1 = gains.at[pl.ds(0, 1)]
    g2 = gains.at[pl.ds(1, 1)]
    g1[...] = g1_in[...].reshape(1, -1)
    g2[...] = g2_in[...].reshape(1, -1)

    def vadd(i, value):
        vbuf[0, pl.ds(i, 1)] = vbuf[0, pl.ds(i, 1)] + value

    def second():
        kinds = lax.broadcasted_iota(jnp.int32, (S_ROW, seqlen), 0)
        for r in range(nrow):
            onehot = (seg[r : r + 1] == kinds).astype(F32)
            count = jnp.sum(onehot, axis=1, keepdims=True)
            share = dpool[r * S_ROW : (r + 1) * S_ROW] / count
            grad[pl.ds(r * seqlen, seqlen)] = dot(onehot, share, 0, 0, HIGH)
        l_cot.wait()
        l_z2.wait()
        l_r2.wait()

        def body(i, _):
            dx = b7[tile(i)].astype(F32) + grad[tile(i)]
            dh, dg, db = norm_grad(dx, b8[tile(i)].astype(F32), rbuf[tile(i), 0:1], g2[...])
            grad[tile(i)] = dh
            b4[tile(i)] = dh.astype(BF)
            vadd(DFG, dg)
            vadd(DFS, db)
            vadd(D2B, jnp.sum(dh, axis=0, keepdims=True))
            return 0

        lax.fori_loop(0, rows // TM, body, 0)
        l_q.start()
        l_k.start()
        l_r1.start()

    def outer(left, right, block):
        def body(i, _):
            cols = pl.ds(pl.multiple_of(i * TM, TM), TM)
            at = pl.multiple_of(block * width + i * TM, TM)
            grads[pl.ds(at, TM)] = dot(left[:, cols], right[...], 0, 0)
            return 0

        lax.fori_loop(0, width // TM, body, 0)

    def ffn_outer(j):
        l_act(j).wait()
        outer(b0, b4, 2 * j)

        @pl.when(j < nff - 1)
        def _():
            l_act(j + 1).start()

        @pl.when(j == nff - 1)
        def _():
            l_z1.start()

    def ffn_inner(j):
        l_w2(j).wait()
        l_dg(j).wait()

        def body(i, _):
            gi = dot(b4[tile(i)], b2[square], 1, 1) * b1[tile(i)].astype(F32)
            b6[tile(i)] = gi.astype(BF)
            vadd(DIB + j, jnp.sum(gi, axis=0, keepdims=True))
            return 0

        lax.fori_loop(0, rows // TM, body, 0)

        @pl.when(j < nff - 1)
        def _():
            l_w2(j + 1).start()
            l_dg(j + 1).start()

    def ffn_dinner(j):
        @pl.when(j == 0)
        def _():
            l_nb.wait()

        outer(b5, b6, 2 * j + 1)

        @pl.when(j == nff - 1)
        def _():
            l_x.start()

    def ffn_back(j):
        l_wi(j).wait()

        def body(i, _):
            grad[tile(i)] = grad[tile(i)] + dot(b6[tile(i)], b3[square], 1, 1)
            return 0

        lax.fori_loop(0, rows // TM, body, 0)

        @pl.when(j < nff - 1)
        def _():
            l_wi(j + 1).start()

        @pl.when(j == nff - 1)
        def _():
            l_c.start()

    def first():
        l_z1.wait()
        l_r1.wait()

        def body(i, _):
            dh, dg, db = norm_grad(grad[tile(i)], b0[tile(i)].astype(F32), rbuf[tile(i), 0:1], g1[...])
            grad[tile(i)] = dh
            b4[tile(i)] = dh.astype(BF)
            vadd(DNG, dg)
            vadd(DNS, db)
            vadd(DOB, jnp.sum(dh, axis=0, keepdims=True))
            return 0

        lax.fori_loop(0, rows // TM, body, 0)

    def project():
        l_c.wait()
        l_wo.wait()
        outer(b6, b4, 2 * nff)

        def body(i, _):
            b3[tile(i)] = dot(b4[tile(i)], b10[square], 1, 1).astype(BF)
            return 0

        lax.fori_loop(0, rows // TM, body, 0)
        l_q.wait()
        l_k.wait()
        l_v.wait()

    parts = halves()

    def attention(a):
        r = a // (pairs // 2)
        span = tile(r, seqlen)
        line = seg[pl.ds(r, 1)]
        bias[...] = jnp.where(column(line) == line, 0.0, masked_score).astype(F32)

        def pair(i, _):
            p = (a - r * (pairs // 2)) * 2 + i
            lanes = pl.ds(pl.multiple_of(p * 128, 128), 128)
            qp = b7[span, lanes] * jnp.asarray(0.125, BF)
            kp = b8[span, lanes]
            vp = b9[span, lanes]
            dc = b3[span, lanes]
            dq = dk = dv = 0.0
            for half, part in enumerate(parts):
                k1 = kp * part
                s = dot(k1, qp, 1, 1) + bias[...]
                prob = jnp.exp(s - lse[(r * pairs + p) * 2 + half])
                dp = dot(vp * part, dc, 1, 1)
                dv = dv + dot(prob.astype(BF), dc * part, 1, 0)
                mean = jnp.sum(prob * dp, axis=0, keepdims=True)
                ds = (prob * (dp - mean)).astype(BF)
                dk = dk + dot(ds, qp * part, 1, 0)
                dq = dq + dot(k1, ds, 0, 0)
            dq = 0.125 * dq.T
            b0[span, lanes] = dq.astype(BF)
            b1[span, lanes] = dk.astype(BF)
            b2[span, lanes] = dv.astype(BF)
            vbuf[0, DQB : DQB + 1, lanes] = vbuf[0, DQB : DQB + 1, lanes] + jnp.sum(dq, axis=0, keepdims=True)
            vbuf[0, DVB : DVB + 1, lanes] = vbuf[0, DVB : DVB + 1, lanes] + jnp.sum(dv, axis=0, keepdims=True)
            return 0

        lax.fori_loop(0, 2, pair, 0)

    def token_part(i):
        out = grad[tile(i)] + dot(b0[tile(i)], b7[square], 1, 1)
        out = out + dot(b1[tile(i)], b8[square], 1, 1)
        grad[tile(i)] = out + dot(b2[tile(i)], b9[square], 1, 1)

    T_LN = 4 * nff - 1
    A0 = T_LN + 2
    A1 = A0 + nrow * pairs // 2
    T_TOK = A1 + 3
    T_END = T_TOK + rows // TM

    def slices(t):
        u = t + 1
        j = u // 4

        for kind, work in enumerate((ffn_outer, ffn_inner, ffn_dinner, ffn_back)):
            @pl.when((u < 4 * nff) & (u - 4 * j == kind))
            def _():
                work(j)

        pl.when(t == T_LN)(first)
        pl.when(t == T_LN + 1)(project)

        @pl.when((t >= A0) & (t < A1))
        def _():
            attention(t - A0)

        @pl.when(t == A1)
        def _():
            l_wq.start()
            l_wk.start()
            l_wv.start()
            l_x.wait()

        for i, src in enumerate((b0, b1, b2)):
            @pl.when(t == A1 + i)
            def _():
                outer(b5, src, 2 * nff + 1 + i)

        @pl.when(t == T_TOK)
        def _():
            l_wq.wait()
            l_wk.wait()
            l_wv.wait()

        @pl.when((t >= T_TOK) & (t < T_END))
        def _():
            token_part(t - T_TOK)

    def pieces(s):
        if s == 0 or S != 5:
            return [(0, width, 0)]
        return [(0, width - NARROW, 0), (width - NARROW, NARROW, 1)]

    def offset(s, c, colour):
        o = c * CH
        for k in range(s):
            o = o + route.bit(k, colour) * (CH >> (k + 1))
        return o

    def reduce_copies(s, c):
        half = CH >> (s + 1)
        here = pl.ds(pl.multiple_of((c % NS) * half, 8), half)
        for i, (x, w, colour) in enumerate(pieces(s)):
            b = route.bit(s, colour)
            o = offset(s, c, colour)
            keep = pl.ds(pl.multiple_of(o + b * half, 8), half)
            send = pl.ds(pl.multiple_of(o + (1 - b) * half, 8), half)
            cols = pl.ds(x, w)
            who = route.partner(s, colour)
            cp = pltpu.make_async_remote_copy(
                grads.at[send, cols], land[s].at[here, cols], ssem.at[s, c, i], rsem.at[s, c, i],
                device_id=who, device_id_type=MESH,
            )
            yield cp, keep, here, cols, who, i

    def gather_copies(s, c):
        half = CH >> (s + 1)
        rank = 2 * S - 1 - s
        for i, (x, w, colour) in enumerate(pieces(s)):
            o = offset(s, c, colour) + route.bit(s, colour) * half
            here = grads.at[pl.ds(pl.multiple_of(o, 8), half), pl.ds(x, w)]
            yield pltpu.make_async_remote_copy(
                here, here, ssem.at[rank, c, i], rsem.at[rank, c, i],
                device_id=route.partner(s, colour), device_id_type=MESH,
            ), i

    def start(p, c):
        if p < S:
            for cp, _, _, _, _, i in reduce_copies(p, c):
                @pl.when(c >= NS)
                def _():
                    pl.semaphore_wait(slot.at[p, c, i], 1)

                cp.start()
        else:
            s = 2 * S - 1 - p
            for cp, i in gather_copies(s, c):
                pl.semaphore_wait(freed.at[s, c, i], 1)
                cp.start()

    def finish(p, c):
        if p < S:
            for cp, keep, here, cols, who, i in reduce_copies(p, c):
                cp.wait_recv()
                grads[keep, cols] = grads[keep, cols] + land[p][here, cols]
                cp.wait_send()
                pl.semaphore_signal(freed.at[p, c, i], inc=1, device_id=who, device_id_type=MESH)

                @pl.when(c + NS < C)
                def _():
                    pl.semaphore_signal(
                        slot.at[p, c + NS, i], inc=1, device_id=who, device_id_type=MESH
                    )
        else:
            for cp, _ in gather_copies(2 * S - 1 - p, c):
                cp.wait()

    def vec_copy(r):
        return pltpu.make_async_remote_copy(
            vbuf.at[r], vrecv.at[r], vs.at[r], vr.at[r], device_id=plain(r), device_id_type=MESH
        )

    NP = 2 * S

    def at(t, p):
        if M == 1:
            c = t - LAG * p
            return c, (c >= 0) & (c < C)
        c = (t - LAG * p + 1) // M - 1
        return c, (c >= 0) & (c < C) & ((c + 1) * M == t - LAG * p + 1)

    def step(t, _):
        for p in range(NP):
            c, valid = at(t, p)
            pl.when(valid)(functools.partial(start, p, c))
        for r in range(S):
            @pl.when(t == T_TOK + 2 * r)
            def _():
                vec_copy(r).start()
        slices(t)
        for p in range(NP):
            c, valid = at(t - FIN, p)
            pl.when(valid)(functools.partial(finish, p, c))
        for r in range(S):
            @pl.when(t == T_TOK + 1 + 2 * r)
            def _():
                cp = vec_copy(r)
                cp.wait()
                vbuf[r + 1] = vbuf[r] + vrecv[r]
        return 0

    second()
    ffn_outer(0)
    pl.semaphore_wait(bar, S)
    steps = max(C * M + LAG * (NP - 1) + FIN, T_TOK + 2 * S, T_END + 1)
    lax.fori_loop(0, steps, step, 0)
    vec_o[...] = vbuf[S]


def backward_reduce(
    tokens, cotangent, kept, weights, lse, segment, dpooled, g1, g2, dp_size, bucket_size
):
    rows, width = tokens.shape
    nrow, seqlen = segment.shape
    wq, wk, wv, wo, wi, w2 = weights
    inner = wi.shape[1]
    nff = inner // width
    dims = bit_dims(dp_size, bucket_size)
    S = len(dims)
    CH = 8 << S
    total = (2 * nff + 4) * width
    C = total // CH
    NS = max(1, 1024 // CH)
    nvec = -(-(8 + nff) // 8) * 8
    vm = pl.BlockSpec(memory_space=pltpu.VMEM)
    hbm = pl.BlockSpec(memory_space=pl.ANY)
    sd = jax.ShapeDtypeStruct
    dma = pltpu.SemaphoreType.DMA
    plain = pltpu.SemaphoreType.REGULAR
    return pl.pallas_call(
        functools.partial(backward_kernel, dims),
        name="backward_reduce",
        out_shape=(
            pltpu.VMEM((total, width), F32), sd((rows, width), F32), sd((nvec, width), F32),
        ),
        in_specs=[hbm] * 19 + [vm] * 5,
        out_specs=[vm, vm, vm],
        scratch_shapes=[pltpu.VMEM((NS * (CH >> (s + 1)), width), F32) for s in range(S)]
        + [pltpu.VMEM((rows, width), BF)] * 11
        + [
            pltpu.VMEM((rows, 128), F32), pltpu.VMEM((seqlen, seqlen), F32),
            pltpu.VMEM((8, width), F32), pltpu.VMEM((S + 1, nvec, width), F32),
            pltpu.VMEM((S, nvec, width), F32),
            dma((4 * nff + 15,)), dma((2 * S, C, 2)), dma((2 * S, C, 2)),
            dma((S,)), dma((S,)), plain((S, C, 2)), plain((S, C, 2)),
        ],
        compiler_params=pltpu.CompilerParams(
            collective_id=1, has_side_effects=True, vmem_limit_bytes=VMEM_KERNEL
        ),
    )(
        tokens, cotangent, *kept, wq, wk, wv, wo, wi, w2, lse, segment, dpooled, g1, g2,
    )


def write_kernel(nff, grads, grad, vec, douter, dinner, dout, dq, dk, dv, tok, *rest):
    sem = rest[-1]
    rest = rest[:-1]
    width = grads.shape[1]

    def block(b):
        return grads.at[pl.ds(b * width, width)]

    copies = [(grad, tok)]
    for j in range(nff):
        copies.append((block(2 * j), douter.at[pl.ds(j * width, width)]))
        copies.append((block(2 * j + 1), dinner.at[:, pl.ds(j * width, width)]))
    for i, dst in enumerate((dout, dq, dk, dv)):
        copies.append((block(2 * nff + i), dst))
    copies = [pltpu.make_async_copy(a, b, sem.at[i]) for i, (a, b) in enumerate(copies)]
    for c in copies:
        c.start()
    at = 0
    for dst in rest:
        for j in range(dst.shape[0] // width):
            dst[pl.ds(j * width, width)] = vec[at]
            at += 1
    for c in copies:
        c.wait()


def write_out(grads, grad, vec, inner):
    width = grads.shape[1]
    nff = inner // width
    sd = jax.ShapeDtypeStruct
    hbm = pl.BlockSpec(memory_space=pl.ANY)
    vm = pl.BlockSpec(memory_space=pltpu.VMEM)
    full = sd((width, width), F32)
    line = sd((width,), F32)
    return pl.pallas_call(
        functools.partial(write_kernel, nff),
        name="write_out",
        out_shape=[sd((inner, width), F32), sd((width, inner), F32), full, full, full, full]
        + [sd(grad.shape, F32)] + [line] * 5 + [sd((inner,), F32)] + [line] * 3,
        in_specs=[hbm, hbm, vm],
        out_specs=[hbm] * 7 + [vm] * 9,
        scratch_shapes=[pltpu.SemaphoreType.DMA((2 * nff + 5,))],
        compiler_params=pltpu.CompilerParams(vmem_limit_bytes=4000000),
    )(grads, grad, vec)


def local(
    dp_size, bucket_size,
    tokens, segment, pair_order, cotangent, query_weight, query_bias, key_weight, value_weight,
    value_bias, out_weight, out_bias, norm_gain, norm_shift, inner_weight, inner_bias,
    outer_weight, outer_bias, final_gain, final_shift,
):
    (
        query_b, key_b, value_b, context_b, normed_b, z1, r1, active_b, slope, z2, r2, lse,
        layer_out, pooled,
    ) = forward(
        tokens, segment, query_weight, query_bias, key_weight, value_weight, value_bias,
        out_weight, out_bias, norm_gain, norm_shift, inner_weight, inner_bias, outer_weight,
        outer_bias, final_gain, final_shift,
    )
    dpooled, loss_value = pair_loss(pooled, pair_order, dp_size, bucket_size)
    loss_value = loss_value.reshape(())
    kept = (
        query_b, key_b, value_b, context_b, normed_b, z1, r1, active_b, slope, z2, r2,
    )
    weights = (query_weight, key_weight, value_weight, out_weight, inner_weight, outer_weight)
    grads, grad, packed = backward_reduce(
        tokens, cotangent, kept, weights, lse, segment, dpooled, norm_gain, final_gain,
        dp_size, bucket_size,
    )
    (
        douter_weight, dinner_weight, dout_weight, dquery_weight, dkey_weight, dvalue_weight,
        tokens_grad, dquery_bias, dvalue_bias, dout_bias, dnorm_gain, dnorm_shift, dinner_bias,
        douter_bias, dfinal_gain, dfinal_shift,
    ) = write_out(grads, grad, packed, inner_bias.shape[0])
    return (
        layer_out, loss_value, tokens_grad, dquery_weight, dquery_bias, dkey_weight,
        dvalue_weight, dvalue_bias, dout_weight, dout_bias, dnorm_gain, dnorm_shift,
        dinner_weight, dinner_bias, douter_weight, douter_bias, dfinal_gain, dfinal_shift,
    )


def solution(mesh):
    split = P(("dp", "bucket"), None)
    return jax.shard_map(
        functools.partial(local, mesh.shape["dp"], mesh.shape["bucket"]),
        mesh=mesh,
        in_specs=(split, split, P(), split) + (P(),) * 15,
        out_specs=(split, P(), split) + (P(),) * 15,
        check_vma=False,
    )
```
